256 devices in a mesh: rows: 256 (over x, y, z, core).
Axes of the slice: x: 4, y: 4, z: 8, core: 2. Of those that a mesh axis runs over, the one named last changes fastest.
Arguments:
- points: float32 [8, 1048576], P(None, 'rows'), may hold values from -6 to 6
- scales: float32 [8], replicated, may hold values from 1 to 3
- noise_var: float32 [1048576], P('rows'), may hold values from 0.05 to 0.5
- pivots: int32 [8, 16], replicated, may hold values from 0 to 1048575, as said below
Outputs:
- factor: float32 [128, 1048576], P(None, 'rows')
- residual_diag: float32 [1048576], P('rows')
- mean_residual: float32 [8], replicated
The draws below stay inside these ranges and needn't reach their ends.
Inputs may be any that keep to these rules, and one draw needn't show every extreme that they name: `pivots`: all 128 entries are distinct point indices.
All inputs are finite; a program needn't handle non-finite values.
Results may differ from the reference program's by a relative error of at most 0.00014.
Values sent between devices are 32-bit elements; how exact they have to be, the bound alone decides.
No kernel may reach another device: no remote copies, remote signals or barrier semaphores. Data moves between devices by JAX's collectives and lax.ppermute only.
A program may use at most 64 MiB of HBM per device.

```python
import math
import jax
import jax.numpy as jnp
from jax import lax

DIM = 8
BS = 16
BLOCKS = 8
NPTS = 1048576


def draw_pivots(key, part):
    chosen = jax.random.permutation(key, NPTS)[:BLOCKS * BS]
    return chosen.reshape((BLOCKS, BS)).astype(jnp.int32)


def block_scale(own_key, extent, split, low, top_value):
    level = 1.0
    for dim, parts in split:
        draws = jax.random.uniform(jax.random.fold_in(jax.random.fold_in(own_key, 6), dim), (parts,), jnp.float32, low / len(split), top_value / len(split))
        level = level * jnp.repeat(jnp.exp(draws), extent[dim] // parts).reshape((-1,) + (1,) * (len(extent) - 1 - dim))
    return level


def centred(own_key, dims, width, reach, split=(), kind=jnp.bfloat16):
    array = jax.random.normal(own_key, dims, jnp.float32) * width
    if len(split) > 0:
        array = block_scale(own_key, dims, split, -0.22, 0.18) * array
    return jnp.clip(array, min=-reach, max=reach).astype(kind)


def setup_inputs(seed: int = 0) -> dict:
    keys = jax.random.split(jax.random.key(seed), 5)
    points = centred(keys[0], (DIM, NPTS), 1.0, 6.0, ((1, 256),), jnp.float32)
    scales = jnp.clip(jnp.exp(jax.random.uniform(keys[1], (DIM,), jnp.float32, math.log(1.0), math.log(3.0))), 1.0, 3.0)
    noise_var = jnp.clip(jnp.exp(math.log(0.5) - 2.3025851 * jax.random.uniform(keys[2], (NPTS,), jnp.float32) ** block_scale(keys[2], (NPTS,), ((0, 256),), -0.2, 0.2)), 0.05, 0.5)
    pivots = draw_pivots(jax.random.fold_in(keys[4], 71), 0)
    return dict(points=points, scales=scales, noise_var=noise_var, pivots=pivots)


def kernel(first_coords, second_coords):
    summed = jnp.zeros((first_coords.shape[1], second_coords.shape[1]), jnp.float32)
    for axis_pos in range(first_coords.shape[0]):
        differ = first_coords[axis_pos][:, None] - second_coords[axis_pos][None, :]
        summed = summed + differ * differ
    return jnp.exp(-0.5 * summed)

def reference(points, scales, noise_var, pivots):
    scaled = points / scales[:, None]
    point_count = points.shape[1]
    point_ids = jnp.arange(point_count, dtype=jnp.int32)
    residual_diag = 1.0 + noise_var
    done_rows = []
    averages = []
    for block_idx in range(BLOCKS):
        wanted = pivots[block_idx]
        pivot_coords = jnp.take(scaled, wanted, axis=1)
        columns = kernel(pivot_coords, scaled) + jnp.where(point_ids[None, :] == wanted[:, None], noise_var[None, :], 0.0)
        for earlier in done_rows:
            picked = jnp.take(earlier, wanted, axis=1)
            columns = columns - jnp.dot(picked.T.astype(jnp.float32), earlier.astype(jnp.float32), precision=lax.Precision.HIGHEST, preferred_element_type=jnp.float32)
        pivot_block = jnp.take(columns, wanted, axis=1)
        chol_block = jnp.linalg.cholesky(pivot_block)
        new_rows = lax.linalg.triangular_solve(chol_block, columns, left_side=True, lower=True)
        done_rows.append(new_rows)
        residual_diag = residual_diag - jnp.sum(new_rows * new_rows, axis=0)
        averages.append(jnp.sum(residual_diag) / point_count)
    return (jnp.concatenate(done_rows, axis=0), residual_diag, jnp.stack(averages))
```

```python
import functools
import math

import jax
import jax.numpy as jnp
from jax import lax
from jax.experimental import pallas as pl
from jax.experimental.pallas import tpu as pltpu
from jax.sharding import Mesh
from jax.sharding import PartitionSpec as P

AXES = ("x", "y", "z", "c")
FIRST = ("x", "y", "c")
SECOND = ("z",)
LANES = 128
SUB = 8
ROOT = math.sqrt(0.5 * math.log2(math.e))
HIGH = lax.Precision.HIGHEST


def iota(shape, dim):
    return lax.broadcasted_iota(jnp.int32, shape, dim)


def splat_row(tile, row):
    return jnp.broadcast_to(tile[row : row + 1, :], tile.shape)


def splat_col(tile, col):
    return jnp.broadcast_to(tile[:, col : col + 1], tile.shape)


def local_pivots(pivots_ref, wide_ref, sizes, point_count):
    blocks, block_rows = pivots_ref.shape
    wide_ref[...] = jnp.zeros_like(wide_ref)
    wide_ref[:, 0:block_rows] = pivots_ref[...]
    lane = iota((SUB, LANES), 1)
    spread = jnp.take_along_axis(wide_ref[...], lane % block_rows, axis=1, mode="promise_in_bounds")
    row = jnp.zeros((SUB, LANES), jnp.int32)
    for block in range(blocks):
        row = jnp.where(lane // block_rows == block, splat_row(spread, block), row)
    index = lax.axis_index(AXES[0])
    for axis in AXES[1:]:
        index = index * sizes[axis] + lax.axis_index(axis)
    return row - index * point_count


def pre_kernel(sizes, copies, points_ref, noise_ref, scales_ref, pivots_ref, send_ref, scaled_ref, local_ref, wide_ref):
    dim, point_count = points_ref.shape
    tiles = point_count // LANES
    local = local_pivots(pivots_ref, wide_ref, sizes, point_count)
    local_ref[...] = local
    sub = iota((SUB, LANES), 0)
    scale = jnp.zeros((SUB, LANES), jnp.float32)
    for d in range(dim):
        scale = jnp.where(sub == d, scales_ref[d], scale)
    factor = ROOT / scale
    owned = (local >= 0) & (local < point_count)
    position = jnp.where(owned, local, -1)
    tile_of = position >> 7
    lane_of = position & (LANES - 1)
    coords = jnp.zeros((SUB, LANES), jnp.float32)
    for t in range(tiles):
        tile = points_ref[:, t * LANES : (t + 1) * LANES] * factor
        scaled_ref[:, t * LANES : (t + 1) * LANES] = tile
        found = jnp.take_along_axis(tile, lane_of, axis=1, mode="promise_in_bounds")
        coords = jnp.where(tile_of == t, found, coords)
    noise = jnp.zeros((SUB, LANES), jnp.float32)
    for a in range(tiles // SUB):
        found = jnp.take_along_axis(noise_ref[a * SUB : (a + 1) * SUB, :], lane_of, axis=1, mode="promise_in_bounds")
        noise = noise + jnp.where(tile_of == sub + a * SUB, found, 0.0)
    noise = jnp.sum(noise, axis=0, keepdims=True)
    for i in range(copies):
        send_ref[i * (dim + 1) : i * (dim + 1) + dim, :] = coords
        send_ref[i * (dim + 1) + dim : (i + 1) * (dim + 1), :] = noise


def main_kernel(
    block_rows, total, got_ref, scaled_ref, noise_ref, local_ref,
    out_ref, resid_ref, sums_ref, bcast_ref, pair_ref, cov_ref,
):
    dim, point_count = scaled_ref.shape
    rank = out_ref.shape[0]
    blocks = rank // block_rows
    halves = block_rows // SUB
    rows = dim + 1
    sub = iota((SUB, LANES), 0)
    lane = iota((SUB, LANES), 1)

    coords = got_ref[0:dim, :]
    noise_p = got_ref[dim:rows, :]
    for i in range(1, got_ref.shape[0] // rows):
        coords = coords + got_ref[i * rows : i * rows + dim, :]
        noise_p = noise_p + got_ref[i * rows + dim : (i + 1) * rows, :]
    local = local_ref[...].astype(jnp.float32)
    columns = jnp.transpose(jnp.concatenate([coords, local], axis=0))
    for d in range(rows):
        bcast_ref[d * rank : (d + 1) * rank, :] = jnp.broadcast_to(columns[:, d : d + 1], (rank, LANES))

    for g in range(rank // SUB):
        total_d = None
        for d in range(dim):
            diff = bcast_ref[d * rank + g * SUB : d * rank + (g + 1) * SUB, :] - splat_row(coords, d)
            total_d = diff * diff if total_d is None else total_d + diff * diff
        block = jnp.exp2(-total_d)
        block = block + jnp.where(lane == sub + g * SUB, jnp.broadcast_to(noise_p, (SUB, LANES)), 0.0)
        pair_ref[g * SUB : (g + 1) * SUB, :] = block

    for k in range(blocks):
        first = k * block_rows
        more = halves if k + 1 < blocks else 0
        tiles = [pair_ref[first + h * SUB : first + (h + 1) * SUB, :] for h in range(halves + more)]
        cols = [[splat_col(tile, first + j) for tile in tiles] for j in range(block_rows)]
        inside = (lane >= first) & (lane < first + block_rows)
        for h in range(halves + more):
            own = jnp.where(lane == sub + first + h * SUB, 1.0, 0.0)
            tiles[h] = jnp.where(inside, own if h < halves else 0.0, tiles[h])
        for m in range(block_rows):
            half, row = divmod(m, SUB)
            inv = lax.rsqrt(splat_row(cols[m][half], row))
            scaled_row = splat_row(tiles[half], row) * inv
            lower = [cols[m][h] * inv if h >= half else None for h in range(halves + more)]
            for j in range(m + 1, block_rows):
                half_j, row_j = divmod(j, SUB)
                entry = splat_row(lower[half_j], row_j)
                for h in range(half_j, halves + more):
                    cols[j][h] = cols[j][h] - lower[h] * entry
            for h in range(half, halves + more):
                if h == half:
                    below = tiles[h] - jnp.where(sub > row, lower[h], 0.0) * scaled_row
                    tiles[h] = jnp.where(sub == row, scaled_row, below)
                else:
                    tiles[h] = tiles[h] - lower[h] * scaled_row
        for h in range(halves + more):
            pair_ref[first + h * SUB : first + (h + 1) * SUB, :] = tiles[h]
        rest = first + 2 * block_rows
        if rest < rank:
            solved = jnp.concatenate(tiles[:halves], axis=0)
            left = jnp.transpose(solved)
            update = jnp.dot(left[rest:, :], solved, precision=HIGH, preferred_element_type=jnp.float32)
            lane_r = iota((rank - rest, LANES), 1)
            inside_r = (lane_r >= first) & (lane_r < first + block_rows)
            pair_ref[rest:, :] = jnp.where(inside_r, 0.0, pair_ref[rest:, :]) - update

    inverse = jnp.where(iota((rank, LANES), 1) <= iota((rank, LANES), 0), pair_ref[...], 0.0)

    width = 2 * LANES
    block_sums = [jnp.zeros((SUB, LANES), jnp.float32) for _ in range(blocks)]

    def step(t, block_sums):
        block_sums = list(block_sums)
        for u in range(width // LANES):
            at = pl.multiple_of(t * width + u * LANES, LANES)
            here = scaled_ref[:, pl.ds(at, LANES)]
            points_d = [splat_row(here, d) for d in range(dim)]
            noise_t = jnp.broadcast_to(noise_ref[pl.ds(t * (width // LANES) + u, 1), :], (SUB, LANES))
            ids = (lane + at).astype(jnp.float32)
            for g in range(rank // SUB):
                total_d = None
                for d in range(dim):
                    diff = bcast_ref[d * rank + g * SUB : d * rank + (g + 1) * SUB, :] - points_d[d]
                    total_d = diff * diff if total_d is None else total_d + diff * diff
                own = bcast_ref[dim * rank + g * SUB : dim * rank + (g + 1) * SUB, :] == ids
                cov_ref[g * SUB : (g + 1) * SUB, u * LANES : (u + 1) * LANES] = jnp.exp2(-total_d) + jnp.where(own, noise_t, 0.0)
        new = jnp.dot(inverse, cov_ref[...], precision=HIGH, preferred_element_type=jnp.float32)
        out_ref[:, pl.ds(pl.multiple_of(t * width, width), width)] = new
        for u in range(width // LANES):
            explained = None
            for b in range(blocks):
                part = None
                for h in range(halves):
                    at = b * block_rows + h * SUB
                    tile = new[at : at + SUB, u * LANES : (u + 1) * LANES]
                    part = tile * tile if part is None else part + tile * tile
                block_sums[b] = block_sums[b] + part
                explained = part if explained is None else explained + part
            row = t * (width // LANES) + u
            resid_ref[pl.ds(row, 1), :] = (1.0 + noise_ref[pl.ds(row, 1), :]) - jnp.sum(explained, axis=0, keepdims=True)
        return tuple(block_sums)

    block_sums = lax.fori_loop(0, point_count // width, step, tuple(block_sums))

    start = None
    for a in range(point_count // LANES // SUB):
        tile = 1.0 + noise_ref[a * SUB : (a + 1) * SUB, :]
        start = tile if start is None else start + tile
    running = start
    means = jnp.zeros((SUB, LANES), jnp.float32)
    for b in range(blocks):
        running = running - block_sums[b]
        means = jnp.where(sub == b, jnp.broadcast_to(jnp.sum(running, axis=0, keepdims=True), (SUB, LANES)), means)
    means = jnp.broadcast_to(jnp.sum(means, axis=1, keepdims=True), (SUB, LANES)) * (1.0 / total)
    sums_ref[...] = jnp.sum(jnp.where(sub == lane, means, 0.0), axis=0, keepdims=True)


def spread(value, axes, count):
    del count
    return lax.all_to_all(value, axes, 0, 0, tiled=False)


def body(sizes, points, scales, noise_var, pivots):
    dim, point_count = points.shape
    blocks, block_rows = pivots.shape
    rank = blocks * block_rows
    devices = math.prod(sizes.values())
    rows = dim + 1
    first = math.prod(sizes[a] for a in FIRST)
    second = math.prod(sizes[a] for a in SECOND)
    noise = noise_var.reshape(point_count // LANES, LANES)
    vmem = pl.BlockSpec(memory_space=pltpu.VMEM)
    smem = pl.BlockSpec(memory_space=pltpu.SMEM)
    send, scaled, local = pl.pallas_call(
        functools.partial(pre_kernel, sizes, first),
        out_shape=(
            jax.ShapeDtypeStruct((first * rows, LANES), jnp.float32),
            jax.ShapeDtypeStruct((dim, point_count), jnp.float32),
            jax.ShapeDtypeStruct((SUB, LANES), jnp.int32),
        ),
        in_specs=[vmem, vmem, smem, vmem],
        out_specs=(vmem, vmem, vmem),
        scratch_shapes=[pltpu.VMEM((SUB, LANES), jnp.int32)],
        name="pick_pivots",
    )(points, noise, scales, pivots)
    got = lax.all_to_all(send.reshape(first, rows, 1, LANES), FIRST, 0, 0)
    got = jnp.sum(got, axis=0)
    got = lax.all_to_all(jnp.broadcast_to(got[None], (second, rows, 1, LANES)), SECOND, 0, 0)
    factor, resid, sums = pl.pallas_call(
        functools.partial(main_kernel, block_rows, devices * point_count),
        out_shape=(
            jax.ShapeDtypeStruct((rank, point_count), jnp.float32),
            jax.ShapeDtypeStruct(noise.shape, jnp.float32),
            jax.ShapeDtypeStruct((1, LANES), jnp.float32),
        ),
        in_specs=[vmem] * 4,
        out_specs=(vmem,) * 3,
        scratch_shapes=[
            pltpu.VMEM((rows * rank, LANES), jnp.float32),
            pltpu.VMEM((rank, LANES), jnp.float32),
            pltpu.VMEM((rank, 2 * LANES), jnp.float32),
        ],
        name="factor_columns",
    )(got.reshape(second * rows, LANES), scaled, noise, local)
    parts = lax.all_to_all(jnp.broadcast_to(sums[None], (devices, 1, LANES)), AXES, 0, 0)
    means = jnp.sum(parts, axis=0)[0, :blocks]
    return factor, resid.reshape(point_count), means


def solution(mesh):
    split = Mesh(mesh.devices.reshape(4, 4, 8, 2), AXES)
    return jax.shard_map(
        functools.partial(body, dict(split.shape)),
        mesh=split,
        in_specs=(P(None, AXES), P(), P(AXES), P()),
        out_specs=(P(None, AXES), P(AXES), P()),
        check_vma=False,
    )
```

```python
import functools
import math

import jax
import jax.numpy as jnp
from jax import lax
from jax.experimental import pallas as pl
from jax.experimental.pallas import tpu as pltpu
from jax.sharding import Mesh
from jax.sharding import PartitionSpec as P

AXES = ("x", "y", "z", "c")
FIRST = ("x", "y", "c")
SECOND = ("z",)
LANES = 128
SUB = 8
ROOT = math.sqrt(0.5 * math.log2(math.e))
HIGH = lax.Precision.HIGHEST


def iota(shape, dim):
    return lax.broadcasted_iota(jnp.int32, shape, dim)


def splat_row(tile, row):
    return jnp.broadcast_to(tile[row : row + 1, :], tile.shape)


def splat_col(tile, col):
    return jnp.broadcast_to(tile[:, col : col + 1], tile.shape)


def local_pivots(pivots_ref, wide_ref, sizes, point_count):
    blocks, block_rows = pivots_ref.shape
    wide_ref[...] = jnp.zeros_like(wide_ref)
    wide_ref[:, 0:block_rows] = pivots_ref[...]
    lane = iota((SUB, LANES), 1)
    spread = jnp.take_along_axis(wide_ref[...], lane % block_rows, axis=1, mode="promise_in_bounds")
    row = jnp.zeros((SUB, LANES), jnp.int32)
    for block in range(blocks):
        row = jnp.where(lane // block_rows == block, splat_row(spread, block), row)
    index = lax.axis_index(AXES[0])
    for axis in AXES[1:]:
        index = index * sizes[axis] + lax.axis_index(axis)
    return row - index * point_count


def pre_kernel(sizes, copies, points_ref, noise_ref, scales_ref, pivots_ref, send_ref, scaled_ref, local_ref, kept_ref, wide_ref):
    dim, point_count = points_ref.shape
    tiles = point_count // LANES
    local = local_pivots(pivots_ref, wide_ref, sizes, point_count)
    local_ref[...] = local
    sub = iota((SUB, LANES), 0)
    scale = jnp.zeros((SUB, LANES), jnp.float32)
    for d in range(dim):
        scale = jnp.where(sub == d, scales_ref[d], scale)
    factor = ROOT / scale
    owned = (local >= 0) & (local < point_count)
    position = jnp.where(owned, local, -1)
    tile_of = position >> 7
    lane_of = position & (LANES - 1)
    coords = jnp.zeros((SUB, LANES), jnp.float32)
    for t in range(tiles):
        tile = points_ref[:, t * LANES : (t + 1) * LANES] * factor
        scaled_ref[:, t * LANES : (t + 1) * LANES] = tile
        found = jnp.take_along_axis(tile, lane_of, axis=1, mode="promise_in_bounds")
        coords = jnp.where(tile_of == t, found, coords)
    kept_ref[...] = noise_ref[...]
    noise = jnp.zeros((SUB, LANES), jnp.float32)
    for a in range(tiles // SUB):
        found = jnp.take_along_axis(noise_ref[a * SUB : (a + 1) * SUB, :], lane_of, axis=1, mode="promise_in_bounds")
        noise = noise + jnp.where(tile_of == sub + a * SUB, found, 0.0)
    noise = jnp.sum(noise, axis=0, keepdims=True)
    for i in range(copies):
        send_ref[i * (dim + 1) : i * (dim + 1) + dim, :] = coords
        send_ref[i * (dim + 1) + dim : (i + 1) * (dim + 1), :] = noise


def covariance_tile(bcast_ref, scaled, noise_row, first_id, dim, rank, group, lane):
    total = None
    for d in range(dim):
        at = d * rank + group * SUB
        diff = bcast_ref[at : at + SUB, :] - scaled[d]
        total = diff * diff if total is None else total + diff * diff
    at = dim * rank + group * SUB
    own = bcast_ref[at : at + SUB, :] == (lane + first_id).astype(jnp.float32)
    return jnp.exp2(-total) + jnp.where(own, noise_row, 0.0)


def main_kernel(
    block_rows, total, got_ref, scaled_ref, noise_ref, local_ref,
    out_hbm, resid_hbm, sums_ref, bcast_ref, pair_ref, cov_ref, out_ref, resid_ref, sems,
):
    dim, point_count = scaled_ref.shape
    rank = pair_ref.shape[0]
    blocks = rank // block_rows
    halves = block_rows // SUB
    rows = dim + 1
    tiles_n = point_count // LANES
    sub = iota((SUB, LANES), 0)
    lane = iota((SUB, LANES), 1)

    coords = got_ref[0:dim, :]
    noise_p = got_ref[dim:rows, :]
    for i in range(1, got_ref.shape[0] // rows):
        coords = coords + got_ref[i * rows : i * rows + dim, :]
        noise_p = noise_p + got_ref[i * rows + dim : (i + 1) * rows, :]
    local = local_ref[...].astype(jnp.float32)
    columns = jnp.transpose(jnp.concatenate([coords, local], axis=0))
    for d in range(rows):
        bcast_ref[d * rank : (d + 1) * rank, :] = jnp.broadcast_to(columns[:, d : d + 1], (rank, LANES))

    for g in range(rank // SUB):
        total_d = None
        for d in range(dim):
            diff = bcast_ref[d * rank + g * SUB : d * rank + (g + 1) * SUB, :] - splat_row(coords, d)
            total_d = diff * diff if total_d is None else total_d + diff * diff
        block = jnp.exp2(-total_d)
        block = block + jnp.where(lane == sub + g * SUB, jnp.broadcast_to(noise_p, (SUB, LANES)), 0.0)
        pair_ref[g * SUB : (g + 1) * SUB, :] = block

    for k in range(blocks):
        first = k * block_rows
        more = halves if k + 1 < blocks else 0
        tiles = [pair_ref[first + h * SUB : first + (h + 1) * SUB, :] for h in range(halves + more)]
        cols = [[splat_col(tile, first + j) for tile in tiles] for j in range(block_rows)]
        inside = (lane >= first) & (lane < first + block_rows)
        for h in range(halves + more):
            own = jnp.where(lane == sub + first + h * SUB, 1.0, 0.0)
            tiles[h] = jnp.where(inside, own if h < halves else 0.0, tiles[h])
        for m in range(block_rows):
            half, row = divmod(m, SUB)
            inv = lax.rsqrt(splat_row(cols[m][half], row))
            scaled_row = splat_row(tiles[half], row) * inv
            lower = [cols[m][h] * inv if h >= half else None for h in range(halves + more)]
            for j in range(m + 1, block_rows):
                half_j, row_j = divmod(j, SUB)
                entry = splat_row(lower[half_j], row_j)
                for h in range(half_j, halves + more):
                    cols[j][h] = cols[j][h] - lower[h] * entry
            for h in range(half, halves + more):
                if h == half:
                    below = tiles[h] - jnp.where(sub > row, lower[h], 0.0) * scaled_row
                    tiles[h] = jnp.where(sub == row, scaled_row, below)
                else:
                    tiles[h] = tiles[h] - lower[h] * scaled_row
        for h in range(halves + more):
            pair_ref[first + h * SUB : first + (h + 1) * SUB, :] = tiles[h]
        for t in range(k * tiles_n // blocks, (k + 1) * tiles_n // blocks):
            here = scaled_ref[:, t * LANES : (t + 1) * LANES]
            scaled = [splat_row(here, d) for d in range(dim)]
            noise_row = jnp.broadcast_to(noise_ref[t : t + 1, :], (SUB, LANES))
            for g in range(rank // SUB):
                tile = covariance_tile(bcast_ref, scaled, noise_row, t * LANES, dim, rank, g, lane)
                cov_ref[g * SUB : (g + 1) * SUB, t * LANES : (t + 1) * LANES] = tile
        rest = first + 2 * block_rows
        if rest < rank:
            solved = jnp.concatenate(tiles[:halves], axis=0)
            left = jnp.transpose(solved)
            update = jnp.dot(left[rest:, :], solved, precision=HIGH, preferred_element_type=jnp.float32)
            lane_r = iota((rank - rest, LANES), 1)
            inside_r = (lane_r >= first) & (lane_r < first + block_rows)
            pair_ref[rest:, :] = jnp.where(inside_r, 0.0, pair_ref[rest:, :]) - update

    inverse = jnp.where(iota((rank, LANES), 1) <= iota((rank, LANES), 0), pair_ref[...], 0.0)

    width = 2 * LANES
    block_sums = [jnp.zeros((SUB, LANES), jnp.float32) for _ in range(blocks)]
    copies = []
    for t in range(point_count // width):
        cols_t = slice(t * width, (t + 1) * width)
        new = jnp.dot(inverse, cov_ref[:, cols_t], precision=HIGH, preferred_element_type=jnp.float32)
        out_ref[:, cols_t] = new
        copy = pltpu.make_async_copy(out_ref.at[:, cols_t], out_hbm.at[:, cols_t], sems.at[t])
        copy.start()
        copies.append(copy)
        for u in range(width // LANES):
            explained = None
            for b in range(blocks):
                part = None
                for h in range(halves):
                    at = b * block_rows + h * SUB
                    tile = new[at : at + SUB, u * LANES : (u + 1) * LANES]
                    part = tile * tile if part is None else part + tile * tile
                block_sums[b] = block_sums[b] + part
                explained = part if explained is None else explained + part
            row = t * (width // LANES) + u
            resid_ref[row : row + 1, :] = (1.0 + noise_ref[row : row + 1, :]) - jnp.sum(explained, axis=0, keepdims=True)
    copy = pltpu.make_async_copy(resid_ref, resid_hbm, sems.at[point_count // width])
    copy.start()
    copies.append(copy)

    running = None
    for a in range(tiles_n // SUB):
        tile = 1.0 + noise_ref[a * SUB : (a + 1) * SUB, :]
        running = tile if running is None else running + tile
    means = jnp.zeros((SUB, LANES), jnp.float32)
    for b in range(blocks):
        running = running - block_sums[b]
        means = jnp.where(sub == b, jnp.broadcast_to(jnp.sum(running, axis=0, keepdims=True), (SUB, LANES)), means)
    means = jnp.broadcast_to(jnp.sum(means, axis=1, keepdims=True), (SUB, LANES)) * (1.0 / total)
    sums_ref[...] = jnp.broadcast_to(jnp.sum(jnp.where(sub == lane, means, 0.0), axis=0, keepdims=True), sums_ref.shape)
    for copy in copies:
        copy.wait()


def body(sizes, points, scales, noise_var, pivots):
    dim, point_count = points.shape
    blocks, block_rows = pivots.shape
    rank = blocks * block_rows
    devices = math.prod(sizes.values())
    rows = dim + 1
    first = math.prod(sizes[a] for a in FIRST)
    second = math.prod(sizes[a] for a in SECOND)
    noise = noise_var.reshape(point_count // LANES, LANES)
    vmem = pl.BlockSpec(memory_space=pltpu.VMEM)
    smem = pl.BlockSpec(memory_space=pltpu.SMEM)
    send, scaled, local, kept = pl.pallas_call(
        functools.partial(pre_kernel, sizes, first),
        out_shape=(
            pltpu.VMEM((first * rows, LANES), jnp.float32),
            pltpu.VMEM((dim, point_count), jnp.float32),
            pltpu.VMEM((SUB, LANES), jnp.int32),
            pltpu.VMEM(noise.shape, jnp.float32),
        ),
        in_specs=[vmem, vmem, smem, vmem],
        out_specs=(vmem,) * 4,
        scratch_shapes=[pltpu.VMEM((SUB, LANES), jnp.int32)],
        name="pick_pivots",
    )(points, noise, scales, pivots)
    got = lax.all_to_all(send.reshape(first, rows, 1, LANES), FIRST, 0, 0)
    got = jnp.sum(got, axis=0)
    got = lax.all_to_all(jnp.broadcast_to(got[None], (second, rows, 1, LANES)), SECOND, 0, 0)
    factor, resid, sums = pl.pallas_call(
        functools.partial(main_kernel, block_rows, devices * point_count),
        out_shape=(
            jax.ShapeDtypeStruct((rank, point_count), jnp.float32),
            jax.ShapeDtypeStruct(noise.shape, jnp.float32),
            pltpu.VMEM((devices, LANES), jnp.float32),
        ),
        in_specs=[vmem] * 4,
        out_specs=(pl.BlockSpec(memory_space=pl.ANY),) * 2 + (vmem,),
        scratch_shapes=[
            pltpu.VMEM((rows * rank, LANES), jnp.float32),
            pltpu.VMEM((rank, LANES), jnp.float32),
            pltpu.VMEM((rank, point_count), jnp.float32),
            pltpu.VMEM((rank, point_count), jnp.float32),
            pltpu.VMEM(noise.shape, jnp.float32),
            pltpu.SemaphoreType.DMA((point_count // (2 * LANES) + 1,)),
        ],
        name="factor_columns",
    )(*(pltpu.with_memory_space_constraint(v, pltpu.VMEM) for v in (got.reshape(second * rows, LANES), scaled, kept, local)))
    parts = lax.all_to_all(sums.reshape(devices, 1, LANES), AXES, 0, 0)
    means = jnp.sum(parts, axis=0)[0, :blocks]
    return factor, resid.reshape(point_count), means


def solution(mesh):
    split = Mesh(mesh.devices.reshape(4, 4, 8, 2), AXES)
    return jax.shard_map(
        functools.partial(body, dict(split.shape)),
        mesh=split,
        in_specs=(P(None, AXES), P(), P(AXES), P()),
        out_specs=(P(None, AXES), P(AXES), P()),
        check_vma=False,
    )
```

```python
import functools
import math

import jax
import jax.numpy as jnp
from jax import lax
from jax.experimental import pallas as pl
from jax.experimental.pallas import tpu as pltpu
from jax.sharding import Mesh
from jax.sharding import PartitionSpec as P

AXES = ("x", "y", "z", "c")
GATHER = (("x", "y"), ("z", "c"))
REDUCE = (("c",), ("x", "y", "z"))
LANES = 128
SUB = 8
ROOT = math.sqrt(0.5 * math.log2(math.e))
HIGH = lax.Precision.HIGHEST
GRID = 16.0


def iota(shape, dim):
    return lax.broadcasted_iota(jnp.int32, shape, dim)


def splat_row(tile, row):
    return jnp.broadcast_to(tile[row : row + 1, :], tile.shape)


def splat_col(tile, col):
    return jnp.broadcast_to(tile[:, col : col + 1], tile.shape)


def local_pivots(pivots_ref, wide_ref, sizes, point_count):
    blocks, block_rows = pivots_ref.shape
    wide_ref[...] = jnp.zeros_like(wide_ref)
    wide_ref[:, 0:block_rows] = pivots_ref[...]
    lane = iota((SUB, LANES), 1)
    spread = jnp.take_along_axis(wide_ref[...], lane % block_rows, axis=1, mode="promise_in_bounds")
    row = jnp.zeros((SUB, LANES), jnp.int32)
    for block in range(blocks):
        row = jnp.where(lane // block_rows == block, splat_row(spread, block), row)
    index = lax.axis_index(AXES[0])
    for axis in AXES[1:]:
        index = index * sizes[axis] + lax.axis_index(axis)
    return row - index * point_count


def pre_kernel(sizes, copies, points_ref, noise_ref, scales_ref, pivots_ref, send_ref, scaled_ref, local_ref, kept_ref, wide_ref):
    dim, point_count = points_ref.shape
    tiles = point_count // LANES
    local = local_pivots(pivots_ref, wide_ref, sizes, point_count)
    local_ref[...] = local
    sub = iota((SUB, LANES), 0)
    scale = jnp.zeros((SUB, LANES), jnp.float32)
    for d in range(dim):
        scale = jnp.where(sub == d, scales_ref[d], scale)
    factor = ROOT / scale
    owned = (local >= 0) & (local < point_count)
    position = jnp.where(owned, local, -1)
    tile_of = position >> 7
    lane_of = position & (LANES - 1)
    coords = jnp.zeros((SUB, LANES), jnp.float32)
    for t in range(tiles):
        tile = points_ref[:, t * LANES : (t + 1) * LANES] * factor
        scaled_ref[:, t * LANES : (t + 1) * LANES] = tile
        found = jnp.take_along_axis(tile, lane_of, axis=1, mode="promise_in_bounds")
        coords = jnp.where(tile_of == t, found, coords)
    kept_ref[...] = noise_ref[...]
    noise = jnp.zeros((SUB, LANES), jnp.float32)
    for a in range(tiles // SUB):
        found = jnp.take_along_axis(noise_ref[a * SUB : (a + 1) * SUB, :], lane_of, axis=1, mode="promise_in_bounds")
        noise = noise + jnp.where(tile_of == sub + a * SUB, found, 0.0)
    noise = jnp.sum(noise, axis=0, keepdims=True)
    for i in range(copies):
        send_ref[i * (dim + 1) : i * (dim + 1) + dim, :] = coords
        send_ref[i * (dim + 1) + dim : (i + 1) * (dim + 1), :] = noise


def pieces(value):
    high = value.astype(jnp.bfloat16)
    value = value - high.astype(jnp.float32)
    middle = value.astype(jnp.bfloat16)
    return high, middle, (value - middle.astype(jnp.float32)).astype(jnp.bfloat16)


def features(coords, second):
    dim, count = coords.shape
    sub = iota((SUB, count), 0)
    coarse = jnp.round(coords * GRID)
    near = coarse * (1.0 / GRID)
    rest = coords - near
    low1 = rest.astype(jnp.bfloat16).astype(jnp.float32)
    left = rest - low1
    low2 = left.astype(jnp.bfloat16).astype(jnp.float32)
    low3 = left - low2
    square = jnp.sum(coarse * coarse, axis=0, keepdims=True)
    square_high = jnp.floor(square * (1.0 / 256)) * 256.0
    square_low = square - square_high
    mixed = jnp.sum(rest * (coords + near), axis=0, keepdims=True)
    mixed1 = mixed.astype(jnp.bfloat16).astype(jnp.float32)
    mixed2 = (mixed - mixed1).astype(jnp.bfloat16).astype(jnp.float32)
    mixed3 = mixed - mixed1 - mixed2

    def rows(*values):
        group = jnp.zeros((SUB, count), jnp.float32)
        for i, value in enumerate(values):
            group = jnp.where(sub == i, value, group)
        return group

    if second:
        return (
            coarse, rows(1.0, 1.0, square_high, square_low),
            low1, low2, low3, low1, low2, low1, near, near, near, rows(1.0, 1.0, 1.0, mixed1, mixed2, mixed3),
        )
    unit = -1.0 / (GRID * GRID)
    two = 2.0 * near
    return (
        coarse * (-2.0 * unit), rows(square_high * unit, square_low * unit, unit, unit),
        two, two, two, 2.0 * low1, 2.0 * low1, 2.0 * low2, 2.0 * low1, 2.0 * low2, 2.0 * low3,
        rows(-mixed1, -mixed2, -mixed3, -1.0, -1.0, -1.0),
    )


def exponent(left, right):
    coarse = jnp.dot(left[:, : 2 * SUB], right[: 2 * SUB, :], preferred_element_type=jnp.float32)
    return coarse + jnp.dot(left[:, 2 * SUB :], right[2 * SUB :, :], preferred_element_type=jnp.float32)


def main_kernel(
    block_rows, total, got_ref, scaled_ref, noise_ref, local_ref,
    out_hbm, resid_hbm, sums_ref, side_ref, pair_ref, cov_ref, out_ref, resid_ref, sems,
):
    dim, point_count = scaled_ref.shape
    rank = pair_ref.shape[0]
    blocks = rank // block_rows
    halves = block_rows // SUB
    rows = dim + 1
    tiles_n = point_count // LANES
    width = 2 * LANES
    sub = iota((SUB, LANES), 0)
    lane = iota((SUB, LANES), 1)

    coords = got_ref[0:dim, :]
    noise_p = got_ref[dim:rows, :]
    for i in range(1, got_ref.shape[0] // rows):
        coords = coords + got_ref[i * rows : i * rows + dim, :]
        noise_p = noise_p + got_ref[i * rows + dim : (i + 1) * rows, :]
    local = local_ref[...].astype(jnp.float32)
    wanted = jnp.broadcast_to(jnp.transpose(local)[:, :1], (rank, LANES))
    pivot_side = jnp.transpose(jnp.concatenate(features(coords, False), axis=0)).astype(jnp.bfloat16)
    own_side = jnp.concatenate(features(coords, True), axis=0).astype(jnp.bfloat16)

    same = iota((rank, LANES), 0) == iota((rank, LANES), 1)
    pair_ref[...] = jnp.where(same, 1.0 + noise_p, jnp.exp2(exponent(pivot_side, own_side)))

    for t in range(tiles_n):
        groups = features(scaled_ref[:, t * LANES : (t + 1) * LANES], True)
        for i in range(0, len(groups), 2):
            pair = jnp.concatenate(groups[i : i + 2], axis=0).astype(jnp.bfloat16)
            side_ref[i * SUB : (i + 2) * SUB, t * LANES : (t + 1) * LANES] = pair

    for k in range(blocks):
        first = k * block_rows
        more = halves if k + 1 < blocks else 0
        tiles = [pair_ref[first + h * SUB : first + (h + 1) * SUB, :] for h in range(halves + more)]
        cols = [[splat_col(tile, first + j) for tile in tiles] for j in range(block_rows)]
        inside = (lane >= first) & (lane < first + block_rows)
        for h in range(halves + more):
            own = jnp.where(lane == sub + first + h * SUB, 1.0, 0.0)
            tiles[h] = jnp.where(inside, own if h < halves else 0.0, tiles[h])
        for m in range(block_rows):
            half, row = divmod(m, SUB)
            inv = lax.rsqrt(splat_row(cols[m][half], row))
            scaled_row = splat_row(tiles[half], row) * inv
            lower = [cols[m][h] * inv if h >= half else None for h in range(halves + more)]
            for j in range(m + 1, block_rows):
                half_j, row_j = divmod(j, SUB)
                entry = splat_row(lower[half_j], row_j)
                for h in range(half_j, halves + more):
                    cols[j][h] = cols[j][h] - lower[h] * entry
            for h in range(half, halves + more):
                if h == half:
                    below = tiles[h] - jnp.where(sub > row, lower[h], 0.0) * scaled_row
                    tiles[h] = jnp.where(sub == row, scaled_row, below)
                else:
                    tiles[h] = tiles[h] - lower[h] * scaled_row
        for h in range(halves + more):
            pair_ref[first + h * SUB : first + (h + 1) * SUB, :] = tiles[h]
        for t in range(k * tiles_n // blocks, (k + 1) * tiles_n // blocks, width // LANES):
            power = exponent(pivot_side, side_ref[:, t * LANES : t * LANES + width])
            for u in range(width // LANES):
                noisy = 1.0 + noise_ref[t + u : t + u + 1, :]
                ids = (iota((rank, LANES), 1) + (t + u) * LANES).astype(jnp.float32)
                tile = jnp.where(wanted == ids, noisy, jnp.exp2(power[:, u * LANES : (u + 1) * LANES]))
                high, middle, low = pieces(tile)
                for i, piece in enumerate((middle, high, low)):
                    cov_ref[i * rank : (i + 1) * rank, (t + u) * LANES : (t + u + 1) * LANES] = piece
        rest = first + 2 * block_rows
        if rest < rank:
            solved = jnp.concatenate(tiles[:halves], axis=0)
            high, middle, low = (piece.astype(jnp.float32) for piece in pieces(solved))
            turned = jnp.transpose(jnp.concatenate([high, high, middle, middle, low, high], axis=0)).astype(jnp.bfloat16)
            flat = jnp.concatenate([high, middle, high, middle, high, low], axis=0).astype(jnp.bfloat16)
            update = jnp.dot(turned[rest:, :], flat, preferred_element_type=jnp.float32)
            lane_r = iota((rank - rest, LANES), 1)
            inside_r = (lane_r >= first) & (lane_r < first + block_rows)
            pair_ref[rest:, :] = jnp.where(inside_r, 0.0, pair_ref[rest:, :]) - update

    inverse = jnp.where(iota((rank, LANES), 1) <= iota((rank, LANES), 0), pair_ref[...], 0.0)

    high, middle, low = pieces(inverse)
    left = jnp.concatenate([high, high, middle, middle, low, high], axis=1)
    block_sums = [jnp.zeros((SUB, LANES), jnp.float32) for _ in range(blocks)]
    copies = []
    for t in range(point_count // width):
        cols_t = slice(t * width, (t + 1) * width)
        large, small = cov_ref[: 2 * rank, cols_t], cov_ref[rank:, cols_t]
        new = jnp.dot(left, jnp.concatenate([large, large, small], axis=0), preferred_element_type=jnp.float32)
        out_ref[:, cols_t] = new
        copy = pltpu.make_async_copy(out_ref.at[:, cols_t], out_hbm.at[:, cols_t], sems.at[t])
        copy.start()
        copies.append(copy)
        for u in range(width // LANES):
            explained = None
            for b in range(blocks):
                part = None
                for h in range(halves):
                    at = b * block_rows + h * SUB
                    tile = new[at : at + SUB, u * LANES : (u + 1) * LANES]
                    part = tile * tile if part is None else part + tile * tile
                block_sums[b] = block_sums[b] + part
                explained = part if explained is None else explained + part
            row = t * (width // LANES) + u
            resid_ref[row : row + 1, :] = (1.0 + noise_ref[row : row + 1, :]) - jnp.sum(explained, axis=0, keepdims=True)
    copy = pltpu.make_async_copy(resid_ref, resid_hbm, sems.at[point_count // width])
    copy.start()
    copies.append(copy)

    running = None
    for a in range(tiles_n // SUB):
        tile = 1.0 + noise_ref[a * SUB : (a + 1) * SUB, :]
        running = tile if running is None else running + tile
    means = jnp.zeros((SUB, LANES), jnp.float32)
    for b in range(blocks):
        running = running - block_sums[b]
        means = jnp.where(sub == b, jnp.broadcast_to(jnp.sum(running, axis=0, keepdims=True), (SUB, LANES)), means)
    means = jnp.broadcast_to(jnp.sum(means, axis=1, keepdims=True), (SUB, LANES)) * (1.0 / total)
    sums_ref[...] = jnp.broadcast_to(jnp.sum(jnp.where(sub == lane, means, 0.0), axis=0, keepdims=True), sums_ref.shape)
    for copy in copies:
        copy.wait()


def exchange(stacked, groups, sizes):
    for i, group in enumerate(groups):
        if i > 0:
            value = jnp.sum(stacked, axis=0)
            stacked = jnp.broadcast_to(value[None], (group_size(group, sizes),) + value.shape)
        if group == ("c",):
            other = lax.ppermute(stacked[0], "c", ((0, 1), (1, 0)))
            stacked = jnp.stack([stacked[0], other])
        else:
            stacked = lax.all_to_all(stacked, group, 0, 0)
    return stacked


def group_size(group, sizes):
    return math.prod(sizes[axis] for axis in group)


def factor_call(block_rows, total, sum_copies, got, scaled, kept, local):
    point_count = scaled.shape[1]
    rank = local.shape[1]
    vmem = pl.BlockSpec(memory_space=pltpu.VMEM)
    hbm = pl.BlockSpec(memory_space=pl.ANY)
    return pl.pallas_call(
        functools.partial(main_kernel, block_rows, total),
        out_shape=(
            jax.ShapeDtypeStruct((rank, point_count), jnp.float32),
            jax.ShapeDtypeStruct(kept.shape, jnp.float32),
            pltpu.VMEM((sum_copies, LANES), jnp.float32),
        ),
        in_specs=[vmem] * 4,
        out_specs=(hbm, hbm, vmem),
        scratch_shapes=[
            pltpu.VMEM((12 * SUB, point_count), jnp.bfloat16),
            pltpu.VMEM((rank, LANES), jnp.float32),
            pltpu.VMEM((3 * rank, point_count), jnp.bfloat16),
            pltpu.VMEM((rank, point_count), jnp.float32),
            pltpu.VMEM(kept.shape, jnp.float32),
            pltpu.SemaphoreType.DMA((point_count // (2 * LANES) + 1,)),
        ],
        name="factor_columns",
    )(*(pltpu.with_memory_space_constraint(v, pltpu.VMEM) for v in (got, scaled, kept, local)))


def body(sizes, points, scales, noise_var, pivots):
    dim, point_count = points.shape
    blocks, block_rows = pivots.shape
    devices = math.prod(sizes.values())
    rows = dim + 1
    copies = group_size(GATHER[0], sizes)
    sum_copies = group_size(REDUCE[0], sizes)
    noise = noise_var.reshape(point_count // LANES, LANES)
    vmem = pl.BlockSpec(memory_space=pltpu.VMEM)
    smem = pl.BlockSpec(memory_space=pltpu.SMEM)
    send, scaled, local, kept = pl.pallas_call(
        functools.partial(pre_kernel, sizes, copies),
        out_shape=(
            pltpu.VMEM((copies * rows, LANES), jnp.float32),
            pltpu.VMEM((dim, point_count), jnp.float32),
            pltpu.VMEM((SUB, LANES), jnp.int32),
            pltpu.VMEM(noise.shape, jnp.float32),
        ),
        in_specs=[vmem, vmem, smem, vmem],
        out_specs=(vmem,) * 4,
        scratch_shapes=[pltpu.VMEM((SUB, LANES), jnp.int32)],
        name="pick_pivots",
    )(points, noise, scales, pivots)
    got = exchange(send.reshape(copies, rows, 1, LANES), GATHER, sizes)
    got = got.reshape(-1, LANES)
    factor, resid, sums = factor_call(block_rows, devices * point_count, sum_copies, got, scaled, kept, local)
    parts = exchange(sums.reshape(sum_copies, 1, LANES), REDUCE, sizes)
    means = jnp.sum(parts, axis=0)[0, :blocks]
    return factor, resid.reshape(point_count), means


def solution(mesh):
    split = Mesh(mesh.devices.reshape(4, 4, 8, 2), AXES)
    return jax.shard_map(
        functools.partial(body, dict(split.shape)),
        mesh=split,
        in_specs=(P(None, AXES), P(), P(AXES), P()),
        out_specs=(P(None, AXES), P(AXES), P()),
        check_vma=False,
    )
```

```python
import functools
import math

import jax
import jax.numpy as jnp
from jax import lax
from jax.experimental import pallas as pl
from jax.experimental.pallas import tpu as pltpu
from jax.sharding import Mesh
from jax.sharding import PartitionSpec as P

AXES = ("x", "y", "z", "c")
GATHER = (("x", "y"), ("z", "c"))
REDUCE = (("c",), ("x", "y", "z"))
LANES = 128
SUB = 8
ROOT = math.sqrt(0.5 * math.log2(math.e))
HIGH = lax.Precision.HIGHEST
GRID = 16.0


def iota(shape, dim):
    return lax.broadcasted_iota(jnp.int32, shape, dim)


def splat_row(tile, row):
    return jnp.broadcast_to(tile[row : row + 1, :], tile.shape)


def splat_col(tile, col):
    return jnp.broadcast_to(tile[:, col : col + 1], tile.shape)


def local_pivots(pivots_ref, wide_ref, sizes, point_count):
    blocks, block_rows = pivots_ref.shape
    wide_ref[...] = jnp.zeros_like(wide_ref)
    wide_ref[:, 0:block_rows] = pivots_ref[...]
    lane = iota((SUB, LANES), 1)
    spread = jnp.take_along_axis(wide_ref[...], lane % block_rows, axis=1, mode="promise_in_bounds")
    row = jnp.zeros((SUB, LANES), jnp.int32)
    for block in range(blocks):
        row = jnp.where(lane // block_rows == block, splat_row(spread, block), row)
    index = lax.axis_index(AXES[0])
    for axis in AXES[1:]:
        index = index * sizes[axis] + lax.axis_index(axis)
    return row - index * point_count


def pre_kernel(sizes, copies, points_ref, noise_ref, scales_ref, pivots_ref, send_ref, scaled_ref, local_ref, kept_ref, wide_ref):
    dim, point_count = points_ref.shape
    tiles = point_count // LANES
    local = local_pivots(pivots_ref, wide_ref, sizes, point_count)
    local_ref[...] = local
    sub = iota((SUB, LANES), 0)
    scale = jnp.zeros((SUB, LANES), jnp.float32)
    for d in range(dim):
        scale = jnp.where(sub == d, scales_ref[d], scale)
    factor = ROOT / scale
    owned = (local >= 0) & (local < point_count)
    position = jnp.where(owned, local, -1)
    tile_of = position >> 7
    lane_of = position & (LANES - 1)
    coords = jnp.zeros((SUB, LANES), jnp.float32)
    for t in range(tiles):
        tile = points_ref[:, t * LANES : (t + 1) * LANES] * factor
        scaled_ref[:, t * LANES : (t + 1) * LANES] = tile
        found = jnp.take_along_axis(tile, lane_of, axis=1, mode="promise_in_bounds")
        coords = jnp.where(tile_of == t, found, coords)
    kept_ref[...] = noise_ref[...]
    noise = jnp.zeros((SUB, LANES), jnp.float32)
    for a in range(tiles // SUB):
        found = jnp.take_along_axis(noise_ref[a * SUB : (a + 1) * SUB, :], lane_of, axis=1, mode="promise_in_bounds")
        noise = noise + jnp.where(tile_of == sub + a * SUB, found, 0.0)
    noise = jnp.sum(noise, axis=0, keepdims=True)
    for i in range(copies):
        send_ref[i * (dim + 1) : i * (dim + 1) + dim, :] = coords
        send_ref[i * (dim + 1) + dim : (i + 1) * (dim + 1), :] = noise


def pieces(value):
    high = value.astype(jnp.bfloat16)
    value = value - high.astype(jnp.float32)
    middle = value.astype(jnp.bfloat16)
    return high, middle, (value - middle.astype(jnp.float32)).astype(jnp.bfloat16)


def features(coords, second):
    dim, count = coords.shape
    sub = iota((SUB, count), 0)
    coarse = jnp.round(coords * GRID)
    near = coarse * (1.0 / GRID)
    rest = coords - near
    low1 = rest.astype(jnp.bfloat16).astype(jnp.float32)
    left = rest - low1
    low2 = left.astype(jnp.bfloat16).astype(jnp.float32)
    low3 = left - low2
    square = jnp.sum(coarse * coarse, axis=0, keepdims=True)
    square_high = jnp.floor(square * (1.0 / 256)) * 256.0
    square_low = square - square_high
    mixed = jnp.sum(rest * (coords + near), axis=0, keepdims=True)
    mixed1 = mixed.astype(jnp.bfloat16).astype(jnp.float32)
    mixed2 = (mixed - mixed1).astype(jnp.bfloat16).astype(jnp.float32)
    mixed3 = mixed - mixed1 - mixed2

    def rows(*values):
        group = jnp.zeros((SUB, count), jnp.float32)
        for i, value in enumerate(values):
            group = jnp.where(sub == i, value, group)
        return group

    if second:
        return (
            coarse, rows(1.0, 1.0, square_high, square_low),
            low1, low2, low3, low1, low2, low1, near, near, near, rows(1.0, 1.0, 1.0, mixed1, mixed2, mixed3),
        )
    unit = -1.0 / (GRID * GRID)
    two = 2.0 * near
    return (
        coarse * (-2.0 * unit), rows(square_high * unit, square_low * unit, unit, unit),
        two, two, two, 2.0 * low1, 2.0 * low1, 2.0 * low2, 2.0 * low1, 2.0 * low2, 2.0 * low3,
        rows(-mixed1, -mixed2, -mixed3, -1.0, -1.0, -1.0),
    )


def exponent(left, right):
    coarse = jnp.dot(left[:, : 2 * SUB], right[: 2 * SUB, :], preferred_element_type=jnp.float32)
    return coarse + jnp.dot(left[:, 2 * SUB :], right[2 * SUB :, :], preferred_element_type=jnp.float32)


def main_kernel(
    block_rows, total, got_ref, scaled_ref, noise_ref, local_ref,
    out_ref, resid_ref, sums_ref, side_ref, pair_ref, cov_ref,
):
    dim, point_count = scaled_ref.shape
    rank = pair_ref.shape[0]
    blocks = rank // block_rows
    halves = block_rows // SUB
    rows = dim + 1
    tiles_n = point_count // LANES
    width = 2 * LANES
    sub = iota((SUB, LANES), 0)
    lane = iota((SUB, LANES), 1)

    coords = got_ref[0:dim, :]
    noise_p = got_ref[dim:rows, :]
    for i in range(1, got_ref.shape[0] // rows):
        coords = coords + got_ref[i * rows : i * rows + dim, :]
        noise_p = noise_p + got_ref[i * rows + dim : (i + 1) * rows, :]
    local = local_ref[...].astype(jnp.float32)
    wanted = jnp.broadcast_to(jnp.transpose(local)[:, :1], (rank, LANES))
    pivot_side = jnp.transpose(jnp.concatenate(features(coords, False), axis=0)).astype(jnp.bfloat16)
    own_side = jnp.concatenate(features(coords, True), axis=0).astype(jnp.bfloat16)

    same = iota((rank, LANES), 0) == iota((rank, LANES), 1)
    pair_ref[...] = jnp.where(same, 1.0 + noise_p, jnp.exp2(exponent(pivot_side, own_side)))

    for t in range(tiles_n):
        groups = features(scaled_ref[:, t * LANES : (t + 1) * LANES], True)
        for i in range(0, len(groups), 2):
            pair = jnp.concatenate(groups[i : i + 2], axis=0).astype(jnp.bfloat16)
            side_ref[i * SUB : (i + 2) * SUB, t * LANES : (t + 1) * LANES] = pair

    for k in range(blocks):
        first = k * block_rows
        more = halves if k + 1 < blocks else 0
        tiles = [pair_ref[first + h * SUB : first + (h + 1) * SUB, :] for h in range(halves + more)]
        cols = [[splat_col(tile, first + j) for tile in tiles] for j in range(block_rows)]
        inside = (lane >= first) & (lane < first + block_rows)
        for h in range(halves + more):
            own = jnp.where(lane == sub + first + h * SUB, 1.0, 0.0)
            tiles[h] = jnp.where(inside, own if h < halves else 0.0, tiles[h])
        for m in range(block_rows):
            half, row = divmod(m, SUB)
            inv = lax.rsqrt(splat_row(cols[m][half], row))
            scaled_row = splat_row(tiles[half], row) * inv
            lower = [cols[m][h] * inv if h >= half else None for h in range(halves + more)]
            for j in range(m + 1, block_rows):
                half_j, row_j = divmod(j, SUB)
                entry = splat_row(lower[half_j], row_j)
                for h in range(half_j, halves + more):
                    cols[j][h] = cols[j][h] - lower[h] * entry
            for h in range(half, halves + more):
                if h == half:
                    below = tiles[h] - jnp.where(sub > row, lower[h], 0.0) * scaled_row
                    tiles[h] = jnp.where(sub == row, scaled_row, below)
                else:
                    tiles[h] = tiles[h] - lower[h] * scaled_row
        for h in range(halves + more):
            pair_ref[first + h * SUB : first + (h + 1) * SUB, :] = tiles[h]
        for t in range(k * tiles_n // blocks, (k + 1) * tiles_n // blocks, width // LANES):
            power = exponent(pivot_side, side_ref[:, t * LANES : t * LANES + width])
            for u in range(width // LANES):
                noisy = 1.0 + noise_ref[t + u : t + u + 1, :]
                ids = (iota((rank, LANES), 1) + (t + u) * LANES).astype(jnp.float32)
                tile = jnp.where(wanted == ids, noisy, jnp.exp2(power[:, u * LANES : (u + 1) * LANES]))
                high, middle, low = pieces(tile)
                for i, piece in enumerate((middle, high, low)):
                    cov_ref[i * rank : (i + 1) * rank, (t + u) * LANES : (t + u + 1) * LANES] = piece
        rest = first + 2 * block_rows
        if rest < rank:
            solved = jnp.concatenate(tiles[:halves], axis=0)
            high, middle, low = (piece.astype(jnp.float32) for piece in pieces(solved))
            turned = jnp.transpose(jnp.concatenate([high, high, middle, middle, low, high], axis=0)).astype(jnp.bfloat16)
            flat = jnp.concatenate([high, middle, high, middle, high, low], axis=0).astype(jnp.bfloat16)
            update = jnp.dot(turned[rest:, :], flat, preferred_element_type=jnp.float32)
            lane_r = iota((rank - rest, LANES), 1)
            inside_r = (lane_r >= first) & (lane_r < first + block_rows)
            pair_ref[rest:, :] = jnp.where(inside_r, 0.0, pair_ref[rest:, :]) - update

    inverse = jnp.where(iota((rank, LANES), 1) <= iota((rank, LANES), 0), pair_ref[...], 0.0)

    high, middle, low = pieces(inverse)
    left = jnp.concatenate([high, high, middle, middle, low, high], axis=1)
    block_sums = [jnp.zeros((SUB, LANES), jnp.float32) for _ in range(blocks)]
    for t in range(point_count // width):
        cols_t = slice(t * width, (t + 1) * width)
        large, small = cov_ref[: 2 * rank, cols_t], cov_ref[rank:, cols_t]
        new = jnp.dot(left, jnp.concatenate([large, large, small], axis=0), preferred_element_type=jnp.float32)
        out_ref[:, cols_t] = new
        for u in range(width // LANES):
            explained = None
            for b in range(blocks):
                part = None
                for h in range(halves):
                    at = b * block_rows + h * SUB
                    tile = new[at : at + SUB, u * LANES : (u + 1) * LANES]
                    part = tile * tile if part is None else part + tile * tile
                block_sums[b] = block_sums[b] + part
                explained = part if explained is None else explained + part
            row = t * (width // LANES) + u
            resid_ref[row : row + 1, :] = (1.0 + noise_ref[row : row + 1, :]) - jnp.sum(explained, axis=0, keepdims=True)

    running = None
    for a in range(tiles_n // SUB):
        tile = 1.0 + noise_ref[a * SUB : (a + 1) * SUB, :]
        running = tile if running is None else running + tile
    means = jnp.zeros((SUB, LANES), jnp.float32)
    for b in range(blocks):
        running = running - block_sums[b]
        means = jnp.where(sub == b, jnp.broadcast_to(jnp.sum(running, axis=0, keepdims=True), (SUB, LANES)), means)
    means = jnp.broadcast_to(jnp.sum(means, axis=1, keepdims=True), (SUB, LANES)) * (1.0 / total)
    sums_ref[...] = jnp.broadcast_to(jnp.sum(jnp.where(sub == lane, means, 0.0), axis=0, keepdims=True), sums_ref.shape)


def exchange(stacked, groups, sizes):
    for i, group in enumerate(groups):
        if i > 0:
            value = jnp.sum(stacked, axis=0)
            stacked = jnp.broadcast_to(value[None], (group_size(group, sizes),) + value.shape)
        if group == ("c",):
            other = lax.ppermute(stacked[0], "c", ((0, 1), (1, 0)))
            stacked = jnp.stack([stacked[0], other])
        else:
            stacked = lax.all_to_all(stacked, group, 0, 0)
    return stacked


def group_size(group, sizes):
    return math.prod(sizes[axis] for axis in group)


def factor_call(block_rows, total, sum_copies, got, scaled, kept, local):
    point_count = scaled.shape[1]
    rank = local.shape[1]
    vmem = pl.BlockSpec(memory_space=pltpu.VMEM)
    return pl.pallas_call(
        functools.partial(main_kernel, block_rows, total),
        out_shape=(
            pltpu.VMEM((rank, point_count), jnp.float32),
            pltpu.VMEM(kept.shape, jnp.float32),
            pltpu.VMEM((sum_copies, LANES), jnp.float32),
        ),
        in_specs=[vmem] * 4,
        out_specs=(vmem,) * 3,
        scratch_shapes=[
            pltpu.VMEM((12 * SUB, point_count), jnp.bfloat16),
            pltpu.VMEM((rank, LANES), jnp.float32),
            pltpu.VMEM((3 * rank, point_count), jnp.bfloat16),
        ],
        compiler_params=pltpu.CompilerParams(vmem_limit_bytes=24 << 20),
        name="factor_columns",
    )(*(pltpu.with_memory_space_constraint(v, pltpu.VMEM) for v in (got, scaled, kept, local)))


def store_kernel(factor_ref, resid_ref, factor_out, resid_out, sems):
    rank = factor_ref.shape[0]
    count = sems.shape[0] - 1
    part = rank // count
    copies = [pltpu.make_async_copy(resid_ref, resid_out, sems.at[count])]
    for i in range(count):
        rows = slice(i * part, (i + 1) * part)
        copies.append(pltpu.make_async_copy(factor_ref.at[rows, :], factor_out.at[rows, :], sems.at[i]))
    for copy in copies:
        copy.start()
    for copy in copies:
        copy.wait()


def store_call(factor, resid):
    vmem = pl.BlockSpec(memory_space=pltpu.VMEM)
    hbm = pl.BlockSpec(memory_space=pl.ANY)
    return pl.pallas_call(
        store_kernel,
        out_shape=(jax.ShapeDtypeStruct(factor.shape, factor.dtype), jax.ShapeDtypeStruct(resid.shape, resid.dtype)),
        in_specs=[vmem] * 2,
        out_specs=(hbm,) * 2,
        scratch_shapes=[pltpu.SemaphoreType.DMA((9,))],
        cost_estimate=pl.CostEstimate(flops=4_000_000_000, bytes_accessed=2 * factor.size * 4, transcendentals=0),
        compiler_params=pltpu.CompilerParams(vmem_limit_bytes=1 << 20),
        name="store_factor",
    )(*(pltpu.with_memory_space_constraint(v, pltpu.VMEM) for v in (factor, resid)))


def body(sizes, points, scales, noise_var, pivots):
    dim, point_count = points.shape
    blocks, block_rows = pivots.shape
    devices = math.prod(sizes.values())
    rows = dim + 1
    copies = group_size(GATHER[0], sizes)
    sum_copies = group_size(REDUCE[0], sizes)
    noise = noise_var.reshape(point_count // LANES, LANES)
    vmem = pl.BlockSpec(memory_space=pltpu.VMEM)
    smem = pl.BlockSpec(memory_space=pltpu.SMEM)
    send, scaled, local, kept = pl.pallas_call(
        functools.partial(pre_kernel, sizes, copies),
        out_shape=(
            pltpu.VMEM((copies * rows, LANES), jnp.float32),
            pltpu.VMEM((dim, point_count), jnp.float32),
            pltpu.VMEM((SUB, LANES), jnp.int32),
            pltpu.VMEM(noise.shape, jnp.float32),
        ),
        in_specs=[vmem, vmem, smem, vmem],
        out_specs=(vmem,) * 4,
        scratch_shapes=[pltpu.VMEM((SUB, LANES), jnp.int32)],
        name="pick_pivots",
    )(points, noise, scales, pivots)
    got = exchange(send.reshape(copies, rows, 1, LANES), GATHER, sizes)
    got = got.reshape(-1, LANES)
    factor, resid, sums = factor_call(block_rows, devices * point_count, sum_copies, got, scaled, kept, local)
    own = sums[:1]
    other = lax.ppermute(own, "c", ((0, 1), (1, 0)))
    factor, resid = store_call(factor, resid)
    both, factor, resid = lax.optimization_barrier((own + other, factor, resid))
    parts = exchange(jnp.broadcast_to(both[None], (group_size(REDUCE[1], sizes), 1, LANES)), REDUCE[1:], sizes)
    means = jnp.sum(parts, axis=0)[0, :blocks]
    return factor, resid.reshape(point_count), means


def solution(mesh):
    split = Mesh(mesh.devices.reshape(4, 4, 8, 2), AXES)
    return jax.shard_map(
        functools.partial(body, dict(split.shape)),
        mesh=split,
        in_specs=(P(None, AXES), P(), P(AXES), P()),
        out_specs=(P(None, AXES), P(AXES), P()),
        check_vma=False,
    )
```

```python
import functools
import math

import jax
import jax.numpy as jnp
from jax import lax
from jax.experimental import pallas as pl
from jax.experimental.pallas import tpu as pltpu
from jax.sharding import Mesh
from jax.sharding import PartitionSpec as P

AXES = ("x", "y", "z", "c")
CHIPS = ("x", "y", "z")
CORES = "c"
LANES = 128
SUB = 8
ROOT = math.sqrt(0.5 * math.log2(math.e))
HIGH = lax.Precision.HIGHEST
GRID = 16.0
SLOTS = 14


def iota(shape, dim):
    return lax.broadcasted_iota(jnp.int32, shape, dim)


def splat_row(tile, row):
    return jnp.broadcast_to(tile[row : row + 1, :], tile.shape)


def splat_col(tile, col):
    return jnp.broadcast_to(tile[:, col : col + 1], tile.shape)


def pivot_row(pivots_ref, wide_ref):
    blocks, block_rows = pivots_ref.shape
    wide_ref[...] = jnp.zeros_like(wide_ref)
    wide_ref[:, 0:block_rows] = pivots_ref[...]
    lane = iota((SUB, LANES), 1)
    spread = jnp.take_along_axis(wide_ref[...], lane % block_rows, axis=1, mode="promise_in_bounds")
    row = jnp.zeros((SUB, LANES), jnp.int32)
    for block in range(blocks):
        row = jnp.where(lane // block_rows == block, splat_row(spread, block), row)
    return row


def chip_index(sizes):
    chip = lax.axis_index(CHIPS[0])
    for axis in CHIPS[1:]:
        chip = chip * sizes[axis] + lax.axis_index(axis)
    return chip


def slots_of_lanes(rank, dim):
    lane = iota((rank, LANES), 1)
    slot = jnp.where(lane < dim * SLOTS, lane // dim, lane - dim * SLOTS)
    return jnp.where(slot < SLOTS, slot, -2 - 2 * rank).astype(jnp.float32)


def message(coords, noise, holds):
    dim = coords.shape[0]
    rank = holds.shape[0]
    index = jnp.sum(jnp.where(holds, iota((rank, LANES), 0) + 1, 0).astype(jnp.float32), axis=0, keepdims=True).astype(jnp.int32)
    index = jnp.broadcast_to(index, (SUB, LANES))
    taken = jnp.maximum(index - 1, 0)
    lane = iota((SUB, LANES), 1)
    place = jnp.where(lane < dim * SLOTS, lane % dim, dim)
    values = jnp.where(iota((SUB, LANES), 0) == place, jnp.take_along_axis(coords, taken, axis=1, mode="promise_in_bounds"), 0.0)
    row = jnp.sum(values, axis=0, keepdims=True)
    noises = jnp.take_along_axis(jnp.broadcast_to(noise, (SUB, LANES)), taken, axis=1, mode="promise_in_bounds")
    row = row + jnp.where(place == dim, noises, 0.0)[:1]
    return jnp.where(index[:1] > 0, row, 0.0)


def pre_kernel(
    sizes, points_hbm, noise_hbm, scales_hbm, pivots_hbm,
    send_ref, values_ref, scaled_ref, about_ref, kept_ref, points_ref, scales_ref, pivots_ref, wide_ref, sems,
):
    copies = []
    for i, (source, target) in enumerate(((pivots_hbm, pivots_ref), (points_hbm, points_ref), (noise_hbm, kept_ref), (scales_hbm, scales_ref))):
        copies.append(pltpu.make_async_copy(source, target, sems.at[i]))
        copies[i].start()
    dim, point_count = points_ref.shape
    tiles = point_count // LANES
    sub = iota((SUB, LANES), 0)
    lane = iota((SUB, LANES), 1)
    chip = chip_index(sizes)

    copies[0].wait()
    pivot = pivot_row(pivots_ref, wide_ref)
    rank = pivots_ref.shape[0] * pivots_ref.shape[1]
    local = pivot - (chip * sizes[CORES] + lax.axis_index(CORES)) * point_count
    owner = pivot // (point_count * sizes[CORES])
    owner_row = jnp.broadcast_to(owner[:1].astype(jnp.float32), (rank, LANES))
    owner_col = jnp.transpose(owner_row)
    same = owner_col == owner_row
    first, second = iota((rank, LANES), 0), iota((rank, LANES), 1)
    place_row = jnp.sum(jnp.where(same & (first < second), 1.0, 0.0), axis=0, keepdims=True)
    place_col = jnp.sum(jnp.where(same & (second < first), 1.0, 0.0), axis=1, keepdims=True)
    place = jnp.broadcast_to(place_row, (SUB, LANES))
    more = jnp.broadcast_to(jnp.max(place, axis=1, keepdims=True), (SUB, LANES)).astype(jnp.int32) // SLOTS
    about_ref[...] = jnp.where(sub == 0, local, jnp.where(sub == 1, owner, jnp.where(sub == 2, place.astype(jnp.int32), more)))
    mine = jnp.where(owner_col == chip.astype(jnp.float32), jnp.broadcast_to(place_col, (rank, LANES)), -1.0 - rank)
    holds = mine == slots_of_lanes(rank, dim)

    owned = (local >= 0) & (local < point_count)
    position = jnp.where(owned, local, -1)
    tile_of = position >> 7
    lane_of = position & (LANES - 1)
    for copy in copies[1:]:
        copy.wait()
    scale = jnp.zeros((SUB, LANES), jnp.float32)
    for d in range(dim):
        scale = jnp.where(sub == d, scales_ref[d], scale)
    factor = ROOT / scale
    coords = jnp.zeros((SUB, LANES), jnp.float32)
    for t in range(tiles):
        tile = points_ref[:, t * LANES : (t + 1) * LANES] * factor
        scaled_ref[:, t * LANES : (t + 1) * LANES] = tile
        found = jnp.take_along_axis(tile, lane_of, axis=1, mode="promise_in_bounds")
        coords = jnp.where(tile_of == t, found, coords)
    noise = jnp.zeros((SUB, LANES), jnp.float32)
    for a in range(tiles // SUB):
        found = jnp.take_along_axis(kept_ref[a * SUB : (a + 1) * SUB, :], lane_of, axis=1, mode="promise_in_bounds")
        noise = noise + jnp.where(tile_of == sub + a * SUB, found, 0.0)
    noise = jnp.sum(noise, axis=0, keepdims=True)
    values_ref[0:dim, :] = coords
    values_ref[dim:, :] = jnp.broadcast_to(noise, (SUB, LANES))
    send_ref[...] = message(coords, noise, holds)


def pack_kernel(sizes, number_ref, values_ref, about_ref, send_ref):
    dim = SUB
    rank = about_ref.shape[1]
    owner = jnp.transpose(jnp.broadcast_to(about_ref[1:2, :], (rank, LANES)).astype(jnp.float32))
    place = jnp.transpose(jnp.broadcast_to(about_ref[2:3, :], (rank, LANES)).astype(jnp.float32))
    first = (number_ref[0] * SLOTS).astype(jnp.float32)
    mine = jnp.where(owner == chip_index(sizes).astype(jnp.float32), place - first, -1.0 - rank)
    send_ref[...] = message(values_ref[0:dim, :], values_ref[dim : dim + 1, :], mine == slots_of_lanes(rank, dim))


def unpack(got, about_ref, number, dim):
    rank = about_ref.shape[1]
    chips = got.shape[0]
    owner = jnp.broadcast_to(about_ref[1:2, :], (chips, rank))
    slot = jnp.broadcast_to(about_ref[2:3, :], (SUB, rank)) - number * SLOTS
    pick = jnp.where(owner == iota((chips, rank), 0), 1.0, 0.0).astype(jnp.bfloat16)
    turned = jnp.concatenate(pieces(jnp.transpose(got)), axis=1)
    picked = jnp.dot(turned, jnp.concatenate([pick] * 3, axis=0), preferred_element_type=jnp.float32)
    coords = jnp.zeros((dim, rank), jnp.float32)
    for s in range(SLOTS):
        coords = jnp.where(slot == s, picked[s * dim : (s + 1) * dim, :], coords)
    noise = jnp.zeros((SUB, rank), jnp.float32)
    sub = iota((SUB, rank), 0)
    for at in range(dim * SLOTS, LANES, SUB):
        noise = noise + jnp.where((slot == sub + (at - dim * SLOTS)) & (slot < SLOTS), picked[at : at + SUB, :], 0.0)
    return coords, jnp.sum(noise, axis=0, keepdims=True)


def unpack_kernel(number_ref, got_ref, about_ref, before_ref, after_ref):
    dim = SUB
    coords, noise = unpack(got_ref[...], about_ref, number_ref[0], dim)
    after_ref[0:dim, :] = before_ref[0:dim, :] + coords
    after_ref[dim:, :] = before_ref[dim:, :] + noise


def pieces(value):
    high = value.astype(jnp.bfloat16)
    value = value - high.astype(jnp.float32)
    middle = value.astype(jnp.bfloat16)
    return high, middle, (value - middle.astype(jnp.float32)).astype(jnp.bfloat16)


def features(coords, second):
    dim, count = coords.shape
    sub = iota((SUB, count), 0)
    coarse = jnp.round(coords * GRID)
    near = coarse * (1.0 / GRID)
    rest = coords - near
    low1 = rest.astype(jnp.bfloat16).astype(jnp.float32)
    left = rest - low1
    low2 = left.astype(jnp.bfloat16).astype(jnp.float32)
    low3 = left - low2
    square = jnp.sum(coarse * coarse, axis=0, keepdims=True)
    square_high = jnp.floor(square * (1.0 / 256)) * 256.0
    square_low = square - square_high
    mixed = jnp.sum(rest * (coords + near), axis=0, keepdims=True)
    mixed1 = mixed.astype(jnp.bfloat16).astype(jnp.float32)
    mixed2 = (mixed - mixed1).astype(jnp.bfloat16).astype(jnp.float32)
    mixed3 = mixed - mixed1 - mixed2

    def rows(*values):
        group = jnp.zeros((SUB, count), jnp.float32)
        for i, value in enumerate(values):
            group = jnp.where(sub == i, value, group)
        return group

    if second:
        return (
            coarse, rows(1.0, 1.0, square_high, square_low),
            low1, low2, low3, low1, low2, low1, near, near, near, rows(1.0, 1.0, 1.0, mixed1, mixed2, mixed3),
        )
    unit = -1.0 / (GRID * GRID)
    two = 2.0 * near
    return (
        coarse * (-2.0 * unit), rows(square_high * unit, square_low * unit, unit, unit),
        two, two, two, 2.0 * low1, 2.0 * low1, 2.0 * low2, 2.0 * low1, 2.0 * low2, 2.0 * low3,
        rows(-mixed1, -mixed2, -mixed3, -1.0, -1.0, -1.0),
    )


def exponent(left, right):
    coarse = jnp.dot(left[:, : 2 * SUB], right[: 2 * SUB, :], preferred_element_type=jnp.float32)
    return coarse + jnp.dot(left[:, 2 * SUB :], right[2 * SUB :, :], preferred_element_type=jnp.float32)


def main_kernel(
    block_rows, total, got_ref, extra_ref, scaled_ref, noise_ref, about_ref,
    out_ref, resid_ref, sums_ref, side_ref, pair_ref, cov_ref,
):
    dim, point_count = scaled_ref.shape
    rank = pair_ref.shape[0]
    blocks = rank // block_rows
    halves = block_rows // SUB
    tiles_n = point_count // LANES
    width = 2 * LANES
    sub = iota((SUB, LANES), 0)
    lane = iota((SUB, LANES), 1)

    coords, noise_p = unpack(got_ref[...], about_ref, 0, dim)
    coords = coords + extra_ref[0:dim, :]
    noise_p = noise_p + extra_ref[dim : dim + 1, :]
    local = jnp.broadcast_to(about_ref[0:1, :], (SUB, LANES)).astype(jnp.float32)
    wanted = jnp.broadcast_to(jnp.transpose(local)[:, :1], (rank, LANES))
    pivot_side = jnp.transpose(jnp.concatenate(features(coords, False), axis=0)).astype(jnp.bfloat16)
    own_side = jnp.concatenate(features(coords, True), axis=0).astype(jnp.bfloat16)

    same = iota((rank, LANES), 0) == iota((rank, LANES), 1)
    pair_ref[...] = jnp.where(same, 1.0 + noise_p, jnp.exp2(exponent(pivot_side, own_side)))

    for t in range(tiles_n):
        groups = features(scaled_ref[:, t * LANES : (t + 1) * LANES], True)
        for i in range(0, len(groups), 2):
            pair = jnp.concatenate(groups[i : i + 2], axis=0).astype(jnp.bfloat16)
            side_ref[i * SUB : (i + 2) * SUB, t * LANES : (t + 1) * LANES] = pair

    for k in range(blocks):
        first = k * block_rows
        more = halves if k + 1 < blocks else 0
        tiles = [pair_ref[first + h * SUB : first + (h + 1) * SUB, :] for h in range(halves + more)]
        cols = [[splat_col(tile, first + j) for tile in tiles] for j in range(block_rows)]
        inside = (lane >= first) & (lane < first + block_rows)
        for h in range(halves + more):
            own = jnp.where(lane == sub + first + h * SUB, 1.0, 0.0)
            tiles[h] = jnp.where(inside, own if h < halves else 0.0, tiles[h])
        for m in range(block_rows):
            half, row = divmod(m, SUB)
            inv = lax.rsqrt(splat_row(cols[m][half], row))
            scaled_row = splat_row(tiles[half], row) * inv
            lower = [cols[m][h] * inv if h >= half else None for h in range(halves + more)]
            for j in range(m + 1, block_rows):
                half_j, row_j = divmod(j, SUB)
                entry = splat_row(lower[half_j], row_j)
                for h in range(half_j, halves + more):
                    cols[j][h] = cols[j][h] - lower[h] * entry
            for h in range(half, halves + more):
                if h == half:
                    below = tiles[h] - jnp.where(sub > row, lower[h], 0.0) * scaled_row
                    tiles[h] = jnp.where(sub == row, scaled_row, below)
                else:
                    tiles[h] = tiles[h] - lower[h] * scaled_row
        for h in range(halves + more):
            pair_ref[first + h * SUB : first + (h + 1) * SUB, :] = tiles[h]
        for t in range(k * tiles_n // blocks, (k + 1) * tiles_n // blocks, width // LANES):
            power = exponent(pivot_side, side_ref[:, t * LANES : t * LANES + width])
            for u in range(width // LANES):
                noisy = 1.0 + noise_ref[t + u : t + u + 1, :]
                ids = (iota((rank, LANES), 1) + (t + u) * LANES).astype(jnp.float32)
                tile = jnp.where(wanted == ids, noisy, jnp.exp2(power[:, u * LANES : (u + 1) * LANES]))
                high, middle, low = pieces(tile)
                for i, piece in enumerate((middle, high, low)):
                    cov_ref[i * rank : (i + 1) * rank, (t + u) * LANES : (t + u + 1) * LANES] = piece
        rest = first + 2 * block_rows
        if rest < rank:
            solved = jnp.concatenate(tiles[:halves], axis=0)
            high, middle, low = (piece.astype(jnp.float32) for piece in pieces(solved))
            turned = jnp.transpose(jnp.concatenate([high, high, middle, middle, low, high], axis=0)).astype(jnp.bfloat16)
            flat = jnp.concatenate([high, middle, high, middle, high, low], axis=0).astype(jnp.bfloat16)
            update = jnp.dot(turned[rest:, :], flat, preferred_element_type=jnp.float32)
            lane_r = iota((rank - rest, LANES), 1)
            inside_r = (lane_r >= first) & (lane_r < first + block_rows)
            pair_ref[rest:, :] = jnp.where(inside_r, 0.0, pair_ref[rest:, :]) - update

    inverse = jnp.where(iota((rank, LANES), 1) <= iota((rank, LANES), 0), pair_ref[...], 0.0)

    high, middle, low = pieces(inverse)
    left = jnp.concatenate([high, high, middle, middle, low, high], axis=1)
    block_sums = [jnp.zeros((SUB, LANES), jnp.float32) for _ in range(blocks)]
    for t in range(point_count // width):
        cols_t = slice(t * width, (t + 1) * width)
        large, small = cov_ref[: 2 * rank, cols_t], cov_ref[rank:, cols_t]
        new = jnp.dot(left, jnp.concatenate([large, large, small], axis=0), preferred_element_type=jnp.float32)
        out_ref[:, cols_t] = new
        for u in range(width // LANES):
            explained = None
            for b in range(blocks):
                part = None
                for h in range(halves):
                    at = b * block_rows + h * SUB
                    tile = new[at : at + SUB, u * LANES : (u + 1) * LANES]
                    part = tile * tile if part is None else part + tile * tile
                block_sums[b] = block_sums[b] + part
                explained = part if explained is None else explained + part
            row = t * (width // LANES) + u
            resid_ref[row : row + 1, :] = (1.0 + noise_ref[row : row + 1, :]) - jnp.sum(explained, axis=0, keepdims=True)

    running = None
    for a in range(tiles_n // SUB):
        tile = 1.0 + noise_ref[a * SUB : (a + 1) * SUB, :]
        running = tile if running is None else running + tile
    means = jnp.zeros((SUB, LANES), jnp.float32)
    for b in range(blocks):
        running = running - block_sums[b]
        means = jnp.where(sub == b, jnp.broadcast_to(jnp.sum(running, axis=0, keepdims=True), (SUB, LANES)), means)
    means = jnp.broadcast_to(jnp.sum(means, axis=1, keepdims=True), (SUB, LANES)) * (1.0 / total)
    sums_ref[...] = jnp.broadcast_to(jnp.sum(jnp.where(sub == lane, means, 0.0), axis=0, keepdims=True), sums_ref.shape)


def factor_call(block_rows, total, *operands):
    point_count = operands[2].shape[1]
    rank = operands[4].shape[1]
    vmem = pl.BlockSpec(memory_space=pltpu.VMEM)
    return pl.pallas_call(
        functools.partial(main_kernel, block_rows, total),
        out_shape=(
            pltpu.VMEM((rank, point_count), jnp.float32),
            pltpu.VMEM((point_count // LANES, LANES), jnp.float32),
            pltpu.VMEM((1, LANES), jnp.float32),
        ),
        in_specs=[vmem] * 5,
        out_specs=(vmem,) * 3,
        scratch_shapes=[
            pltpu.VMEM((12 * SUB, point_count), jnp.bfloat16),
            pltpu.VMEM((rank, LANES), jnp.float32),
            pltpu.VMEM((3 * rank, point_count), jnp.bfloat16),
        ],
        compiler_params=pltpu.CompilerParams(vmem_limit_bytes=24 << 20),
        name="factor_columns",
    )(*in_vmem(*operands))


def in_vmem(*values):
    return [pltpu.with_memory_space_constraint(value, pltpu.VMEM) for value in values]


def store_kernel(factor_ref, resid_ref, factor_out, resid_out, sems):
    rank = factor_ref.shape[0]
    count = sems.shape[0] - 1
    part = rank // count
    copies = [pltpu.make_async_copy(resid_ref, resid_out, sems.at[count])]
    for i in range(count):
        rows = slice(i * part, (i + 1) * part)
        copies.append(pltpu.make_async_copy(factor_ref.at[rows, :], factor_out.at[rows, :], sems.at[i]))
    for copy in copies:
        copy.start()
    for copy in copies:
        copy.wait()


def store_call(factor, resid):
    vmem = pl.BlockSpec(memory_space=pltpu.VMEM)
    hbm = pl.BlockSpec(memory_space=pl.ANY)
    return pl.pallas_call(
        store_kernel,
        out_shape=(jax.ShapeDtypeStruct(factor.shape, factor.dtype), jax.ShapeDtypeStruct(resid.shape, resid.dtype)),
        in_specs=[vmem] * 2,
        out_specs=(hbm,) * 2,
        scratch_shapes=[pltpu.SemaphoreType.DMA((9,))],
        cost_estimate=pl.CostEstimate(flops=4_000_000_000, bytes_accessed=2 * factor.size * 4, transcendentals=0),
        compiler_params=pltpu.CompilerParams(vmem_limit_bytes=1 << 20),
        name="store_factor",
    )(*in_vmem(factor, resid))


def to_chips(row, sizes):
    chips = math.prod(sizes[axis] for axis in CHIPS)
    return lax.all_to_all(jnp.broadcast_to(row[None], (chips,) + row.shape), CHIPS, 0, 0)


def of_chip(row):
    return row + lax.ppermute(row, CORES, ((0, 1), (1, 0)))


def body(sizes, points, scales, noise_var, pivots):
    dim, point_count = points.shape
    blocks, block_rows = pivots.shape
    devices = math.prod(sizes.values())
    chips = devices // sizes[CORES]
    noise = noise_var.reshape(point_count // LANES, LANES)
    vmem = pl.BlockSpec(memory_space=pltpu.VMEM)
    smem = pl.BlockSpec(memory_space=pltpu.SMEM)
    hbm = pl.BlockSpec(memory_space=pl.ANY)
    send, values, scaled, about, kept = pl.pallas_call(
        functools.partial(pre_kernel, sizes),
        out_shape=(
            pltpu.VMEM((1, LANES), jnp.float32),
            pltpu.VMEM((2 * SUB, LANES), jnp.float32),
            pltpu.VMEM((dim, point_count), jnp.float32),
            pltpu.VMEM((SUB, LANES), jnp.int32),
            pltpu.VMEM(noise.shape, jnp.float32),
        ),
        in_specs=[hbm] * 4,
        out_specs=(vmem,) * 5,
        scratch_shapes=[
            pltpu.VMEM((dim, point_count), jnp.float32),
            pltpu.SMEM((dim,), jnp.float32),
            pltpu.VMEM((blocks, block_rows), jnp.int32),
            pltpu.VMEM((SUB, LANES), jnp.int32),
            pltpu.SemaphoreType.DMA((4,)),
        ],
        name="pick_pivots",
    )(points, noise, scales, pivots)
    row = of_chip(send)
    last, row = lax.optimization_barrier((about[3, 0], row))
    got = to_chips(row, sizes).reshape(chips, LANES)

    def another(state):
        number, end, extra = state
        packed = pl.pallas_call(
            functools.partial(pack_kernel, sizes),
            out_shape=jax.ShapeDtypeStruct((1, LANES), jnp.float32),
            in_specs=[smem] + [vmem] * 2,
            out_specs=vmem,
            name="pack_more",
        )(number[None], values, about)
        more_got = to_chips(of_chip(packed), sizes).reshape(chips, LANES)
        extra = pl.pallas_call(
            unpack_kernel,
            out_shape=jax.ShapeDtypeStruct(extra.shape, jnp.float32),
            in_specs=[smem] + [vmem] * 3,
            out_specs=vmem,
            name="unpack_more",
        )(number[None], more_got, about, extra)
        return number + 1, end, extra

    start = (jnp.int32(1), last, jnp.zeros((2 * SUB, LANES), jnp.float32))
    extra = lax.while_loop(lambda state: state[0] <= state[1], another, start)[2]

    factor, resid, sums = factor_call(block_rows, devices * point_count, got, extra, scaled, kept, about)
    both = of_chip(sums)
    factor, resid = store_call(factor, resid)
    both, factor, resid = lax.optimization_barrier((both, factor, resid))
    means = jnp.sum(to_chips(both, sizes), axis=0)[0, :blocks]
    return factor, resid.reshape(point_count), means


def solution(mesh):
    split = Mesh(mesh.devices.reshape(4, 4, 8, 2), AXES)
    return jax.shard_map(
        functools.partial(body, dict(split.shape)),
        mesh=split,
        in_specs=(P(None, AXES), P(), P(AXES), P()),
        out_specs=(P(None, AXES), P(AXES), P()),
        check_vma=False,
    )
```

```python
import functools
import math

import jax
import jax.numpy as jnp
from jax import lax
from jax.experimental import pallas as pl
from jax.experimental.pallas import tpu as pltpu
from jax.sharding import Mesh
from jax.sharding import PartitionSpec as P


AXES = ("x", "y", "z", "c")
CHIPS = ("x", "y", "z")
CORES = "c"
LANES = 128
SUB = 8
ROOT = math.sqrt(0.5 * math.log2(math.e))
GRID = 16.0
SLOTS = 14


def iota(shape, dim):
    return lax.broadcasted_iota(jnp.int32, shape, dim)


def splat_row(tile, row):
    return jnp.broadcast_to(tile[row : row + 1, :], tile.shape)


def splat_col(tile, col):
    return jnp.broadcast_to(tile[:, col : col + 1], tile.shape)


def pivot_row(pivots_ref, wide_ref):
    blocks, block_rows = pivots_ref.shape
    wide_ref[...] = jnp.zeros_like(wide_ref)
    wide_ref[:, 0:block_rows] = pivots_ref[...]
    lane = iota((SUB, LANES), 1)
    spread = jnp.take_along_axis(wide_ref[...], lane % block_rows, axis=1, mode="promise_in_bounds")
    row = jnp.zeros((SUB, LANES), jnp.int32)
    for block in range(blocks):
        row = jnp.where(lane // block_rows == block, splat_row(spread, block), row)
    return row


def chip_index(sizes):
    chip = lax.axis_index(CHIPS[0])
    for axis in CHIPS[1:]:
        chip = chip * sizes[axis] + lax.axis_index(axis)
    return chip


def slots_of_lanes(rank, dim):
    lane = iota((rank, LANES), 1)
    slot = jnp.where(lane < dim * SLOTS, lane // dim, lane - dim * SLOTS)
    return jnp.where(slot < SLOTS, slot, -2 - 2 * rank).astype(jnp.float32)


def message(coords, noise, holds):
    dim = coords.shape[0]
    rank = holds.shape[0]
    index = jnp.sum(jnp.where(holds, iota((rank, LANES), 0) + 1, 0).astype(jnp.float32), axis=0, keepdims=True).astype(jnp.int32)
    index = jnp.broadcast_to(index, (SUB, LANES))
    taken = jnp.maximum(index - 1, 0)
    lane = iota((SUB, LANES), 1)
    place = jnp.where(lane < dim * SLOTS, lane % dim, dim)
    values = jnp.where(iota((SUB, LANES), 0) == place, jnp.take_along_axis(coords, taken, axis=1, mode="promise_in_bounds"), 0.0)
    row = jnp.sum(values, axis=0, keepdims=True)
    noises = jnp.take_along_axis(jnp.broadcast_to(noise, (SUB, LANES)), taken, axis=1, mode="promise_in_bounds")
    row = row + jnp.where(place == dim, noises, 0.0)[:1]
    return jnp.where(index[:1] > 0, row, 0.0)


def pre_kernel(
    sizes, points_hbm, noise_hbm, scales_hbm, pivots_hbm,
    send_ref, values_ref, scaled_ref, about_ref, kept_ref, points_ref, scales_ref, pivots_ref, wide_ref, sems,
):
    copies = []
    for i, (source, target) in enumerate(((pivots_hbm, pivots_ref), (points_hbm, points_ref), (noise_hbm, kept_ref), (scales_hbm, scales_ref))):
        copies.append(pltpu.make_async_copy(source, target, sems.at[i]))
        copies[i].start()
    dim, point_count = points_ref.shape
    tiles = point_count // LANES
    sub = iota((SUB, LANES), 0)
    lane = iota((SUB, LANES), 1)
    chip = chip_index(sizes)

    copies[0].wait()
    pivot = pivot_row(pivots_ref, wide_ref)
    rank = pivots_ref.shape[0] * pivots_ref.shape[1]
    local = pivot - (chip * sizes[CORES] + lax.axis_index(CORES)) * point_count
    owner = pivot // (point_count * sizes[CORES])
    owner_row = jnp.broadcast_to(owner[:1].astype(jnp.float32), (rank, LANES))
    owner_col = jnp.transpose(owner_row)
    same = owner_col == owner_row
    first, second = iota((rank, LANES), 0), iota((rank, LANES), 1)
    place_row = jnp.sum(jnp.where(same & (first < second), 1.0, 0.0), axis=0, keepdims=True)
    place_col = jnp.sum(jnp.where(same & (second < first), 1.0, 0.0), axis=1, keepdims=True)
    place = jnp.broadcast_to(place_row, (SUB, LANES))
    more = jnp.broadcast_to(jnp.max(place, axis=1, keepdims=True), (SUB, LANES)).astype(jnp.int32) // SLOTS
    about_ref[...] = jnp.where(sub == 0, local, jnp.where(sub == 1, owner, jnp.where(sub == 2, place.astype(jnp.int32), more)))
    mine = jnp.where(owner_col == chip.astype(jnp.float32), jnp.broadcast_to(place_col, (rank, LANES)), -1.0 - rank)
    holds = mine == slots_of_lanes(rank, dim)

    owned = (local >= 0) & (local < point_count)
    position = jnp.where(owned, local, -1)
    tile_of = position >> 7
    lane_of = position & (LANES - 1)
    for copy in copies[1:]:
        copy.wait()
    scale = jnp.zeros((SUB, LANES), jnp.float32)
    for d in range(dim):
        scale = jnp.where(sub == d, scales_ref[d], scale)
    factor = ROOT / scale
    coords = jnp.zeros((SUB, LANES), jnp.float32)
    for t in range(tiles):
        tile = points_ref[:, t * LANES : (t + 1) * LANES] * factor
        scaled_ref[:, t * LANES : (t + 1) * LANES] = tile
        found = jnp.take_along_axis(tile, lane_of, axis=1, mode="promise_in_bounds")
        coords = jnp.where(tile_of == t, found, coords)
    noise = jnp.zeros((SUB, LANES), jnp.float32)
    for a in range(tiles // SUB):
        found = jnp.take_along_axis(kept_ref[a * SUB : (a + 1) * SUB, :], lane_of, axis=1, mode="promise_in_bounds")
        noise = noise + jnp.where(tile_of == sub + a * SUB, found, 0.0)
    noise = jnp.sum(noise, axis=0, keepdims=True)
    values_ref[0:dim, :] = coords
    values_ref[dim:, :] = jnp.broadcast_to(noise, (SUB, LANES))
    send_ref[...] = message(coords, noise, holds)


def pack_kernel(sizes, number_ref, values_ref, about_ref, send_ref):
    dim = SUB
    rank = about_ref.shape[1]
    owner = jnp.transpose(jnp.broadcast_to(about_ref[1:2, :], (rank, LANES)).astype(jnp.float32))
    place = jnp.transpose(jnp.broadcast_to(about_ref[2:3, :], (rank, LANES)).astype(jnp.float32))
    first = (number_ref[0] * SLOTS).astype(jnp.float32)
    mine = jnp.where(owner == chip_index(sizes).astype(jnp.float32), place - first, -1.0 - rank)
    send_ref[...] = message(values_ref[0:dim, :], values_ref[dim : dim + 1, :], mine == slots_of_lanes(rank, dim))


def unpack(got, about_ref, number, dim):
    rank = about_ref.shape[1]
    chips = got.shape[0]
    owner = jnp.broadcast_to(about_ref[1:2, :], (chips, rank))
    slot = jnp.broadcast_to(about_ref[2:3, :], (SUB, rank)) - number * SLOTS
    pick = jnp.where(owner == iota((chips, rank), 0), 1.0, 0.0).astype(jnp.bfloat16)
    turned = jnp.concatenate(pieces(jnp.transpose(got)), axis=1)
    picked = jnp.dot(turned, jnp.concatenate([pick] * 3, axis=0), preferred_element_type=jnp.float32)
    coords = jnp.zeros((dim, rank), jnp.float32)
    for s in range(SLOTS):
        coords = jnp.where(slot == s, picked[s * dim : (s + 1) * dim, :], coords)
    noise = jnp.zeros((SUB, rank), jnp.float32)
    sub = iota((SUB, rank), 0)
    for at in range(dim * SLOTS, LANES, SUB):
        noise = noise + jnp.where((slot == sub + (at - dim * SLOTS)) & (slot < SLOTS), picked[at : at + SUB, :], 0.0)
    return coords, jnp.sum(noise, axis=0, keepdims=True)


def unpack_kernel(number_ref, got_ref, about_ref, before_ref, after_ref):
    dim = SUB
    coords, noise = unpack(got_ref[...], about_ref, number_ref[0], dim)
    after_ref[0:dim, :] = before_ref[0:dim, :] + coords
    after_ref[dim:, :] = before_ref[dim:, :] + noise


def pieces(value):
    high = value.astype(jnp.bfloat16)
    value = value - high.astype(jnp.float32)
    middle = value.astype(jnp.bfloat16)
    return high, middle, (value - middle.astype(jnp.float32)).astype(jnp.bfloat16)


def features(coords, second):
    _, count = coords.shape
    sub = iota((SUB, count), 0)
    coarse = jnp.round(coords * GRID)
    near = coarse * (1.0 / GRID)
    rest = coords - near
    low1 = rest.astype(jnp.bfloat16).astype(jnp.float32)
    left = rest - low1
    low2 = left.astype(jnp.bfloat16).astype(jnp.float32)
    low3 = left - low2
    square = jnp.sum(coarse * coarse, axis=0, keepdims=True)
    square_high = jnp.floor(square * (1.0 / 256)) * 256.0
    square_low = square - square_high
    mixed = jnp.sum(rest * (coords + near), axis=0, keepdims=True)
    mixed1 = mixed.astype(jnp.bfloat16).astype(jnp.float32)
    mixed2 = (mixed - mixed1).astype(jnp.bfloat16).astype(jnp.float32)
    mixed3 = mixed - mixed1 - mixed2

    def rows(*values):
        group = jnp.zeros((SUB, count), jnp.float32)
        for i, value in enumerate(values):
            group = jnp.where(sub == i, value, group)
        return group

    if second:
        return (
            coarse, rows(1.0, 1.0, square_high, square_low),
            low1, low2, low3, low1, low2, low1, near, near, near, rows(1.0, 1.0, 1.0, mixed1, mixed2, mixed3),
        )
    unit = -1.0 / (GRID * GRID)
    two = 2.0 * near
    return (
        coarse * (-2.0 * unit), rows(square_high * unit, square_low * unit, unit, unit),
        two, two, two, 2.0 * low1, 2.0 * low1, 2.0 * low2, 2.0 * low1, 2.0 * low2, 2.0 * low3,
        rows(-mixed1, -mixed2, -mixed3, -1.0, -1.0, -1.0),
    )


def exponent(left, right):
    return jnp.dot(left, right, preferred_element_type=jnp.float32)


def main_kernel(
    block_rows, total, got_ref, extra_ref, scaled_ref, noise_ref, about_ref,
    out_ref, resid_ref, sums_ref, side_ref, pair_ref, cov_ref,
):
    dim, point_count = scaled_ref.shape
    rank = pair_ref.shape[0]
    blocks = rank // block_rows
    halves = block_rows // SUB
    tiles_n = point_count // LANES
    width = 2 * LANES
    sub = iota((SUB, LANES), 0)
    lane = iota((SUB, LANES), 1)

    coords, noise_p = unpack(got_ref[...], about_ref, 0, dim)
    coords = coords + extra_ref[0:dim, :]
    noise_p = noise_p + extra_ref[dim : dim + 1, :]
    local = jnp.broadcast_to(about_ref[0:1, :], (SUB, LANES)).astype(jnp.float32)
    wanted = jnp.broadcast_to(jnp.transpose(local)[:, :1], (rank, LANES))
    pivot_side = jnp.transpose(jnp.concatenate(features(coords, False), axis=0)).astype(jnp.bfloat16)
    own_side = jnp.concatenate(features(coords, True), axis=0).astype(jnp.bfloat16)

    same = iota((rank, LANES), 0) == iota((rank, LANES), 1)
    pair_ref[...] = jnp.where(same, 1.0 + noise_p, jnp.exp2(exponent(pivot_side, own_side)))

    for t in range(tiles_n):
        groups = features(scaled_ref[:, t * LANES : (t + 1) * LANES], True)
        for i in range(0, len(groups), 2):
            pair = jnp.concatenate(groups[i : i + 2], axis=0).astype(jnp.bfloat16)
            side_ref[i * SUB : (i + 2) * SUB, t * LANES : (t + 1) * LANES] = pair

    for k in range(blocks):
        first = k * block_rows
        more = halves if k + 1 < blocks else 0
        tiles = [pair_ref[first + h * SUB : first + (h + 1) * SUB, :] for h in range(halves + more)]
        cols = [[splat_col(tile, first + j) for tile in tiles] for j in range(block_rows)]
        inside = (lane >= first) & (lane < first + block_rows)
        for h in range(halves + more):
            own = jnp.where(lane == sub + first + h * SUB, 1.0, 0.0)
            tiles[h] = jnp.where(inside, own if h < halves else 0.0, tiles[h])
        for m in range(block_rows):
            half, row = divmod(m, SUB)
            inv = lax.rsqrt(splat_row(cols[m][half], row))
            scaled_row = splat_row(tiles[half], row) * inv
            lower = [cols[m][h] * inv if h >= half else None for h in range(halves + more)]
            for j in range(m + 1, block_rows):
                half_j, row_j = divmod(j, SUB)
                entry = splat_row(lower[half_j], row_j)
                for h in range(half_j, halves + more):
                    cols[j][h] = cols[j][h] - lower[h] * entry
            for h in range(half, halves + more):
                if h == half:
                    below = tiles[h] - jnp.where(sub > row, lower[h], 0.0) * scaled_row
                    tiles[h] = jnp.where(sub == row, scaled_row, below)
                else:
                    tiles[h] = tiles[h] - lower[h] * scaled_row
        for h in range(halves + more):
            pair_ref[first + h * SUB : first + (h + 1) * SUB, :] = tiles[h]
        for t in range(k * tiles_n // blocks, (k + 1) * tiles_n // blocks, width // LANES):
            power = exponent(pivot_side, side_ref[:, t * LANES : t * LANES + width])
            for u in range(width // LANES):
                noisy = 1.0 + noise_ref[t + u : t + u + 1, :]
                ids = (iota((rank, LANES), 1) + (t + u) * LANES).astype(jnp.float32)
                tile = jnp.where(wanted == ids, noisy, jnp.exp2(power[:, u * LANES : (u + 1) * LANES]))
                high, middle, low = pieces(tile)
                for i, piece in enumerate((middle, high, low)):
                    cov_ref[i * rank : (i + 1) * rank, (t + u) * LANES : (t + u + 1) * LANES] = piece
        rest = first + 2 * block_rows
        if rest < rank:
            solved = jnp.concatenate(tiles[:halves], axis=0)
            high, middle, low = (piece.astype(jnp.float32) for piece in pieces(solved))
            turned = jnp.transpose(jnp.concatenate([high, high, middle, middle, low, high], axis=0)).astype(jnp.bfloat16)
            flat = jnp.concatenate([high, middle, high, middle, high, low], axis=0).astype(jnp.bfloat16)
            update = jnp.dot(turned[rest:, :], flat, preferred_element_type=jnp.float32)
            lane_r = iota((rank - rest, LANES), 1)
            inside_r = (lane_r >= first) & (lane_r < first + block_rows)
            pair_ref[rest:, :] = jnp.where(inside_r, 0.0, pair_ref[rest:, :]) - update

    inverse = jnp.where(iota((rank, LANES), 1) <= iota((rank, LANES), 0), pair_ref[...], 0.0)

    high, middle, low = pieces(inverse)
    left = jnp.concatenate([high, high, middle, middle, low, high], axis=1)
    block_sums = [jnp.zeros((SUB, LANES), jnp.float32) for _ in range(blocks)]
    for t in range(point_count // width):
        cols_t = slice(t * width, (t + 1) * width)
        large, small = cov_ref[: 2 * rank, cols_t], cov_ref[rank:, cols_t]
        new = jnp.dot(left, jnp.concatenate([large, large, small], axis=0), preferred_element_type=jnp.float32)
        out_ref[:, cols_t] = new
        for u in range(width // LANES):
            explained = None
            for b in range(blocks):
                part = None
                for h in range(halves):
                    at = b * block_rows + h * SUB
                    tile = new[at : at + SUB, u * LANES : (u + 1) * LANES]
                    part = tile * tile if part is None else part + tile * tile
                block_sums[b] = block_sums[b] + part
                explained = part if explained is None else explained + part
            row = t * (width // LANES) + u
            resid_ref[row : row + 1, :] = (1.0 + noise_ref[row : row + 1, :]) - jnp.sum(explained, axis=0, keepdims=True)

    running = None
    for a in range(tiles_n // SUB):
        tile = 1.0 + noise_ref[a * SUB : (a + 1) * SUB, :]
        running = tile if running is None else running + tile
    means = jnp.zeros((SUB, LANES), jnp.float32)
    for b in range(blocks):
        running = running - block_sums[b]
        means = jnp.where(sub == b, jnp.broadcast_to(jnp.sum(running, axis=0, keepdims=True), (SUB, LANES)), means)
    means = jnp.broadcast_to(jnp.sum(means, axis=1, keepdims=True), (SUB, LANES)) * (1.0 / total)
    sums_ref[...] = jnp.broadcast_to(jnp.sum(jnp.where(sub == lane, means, 0.0), axis=0, keepdims=True), sums_ref.shape)


def factor_call(block_rows, total, *operands):
    point_count = operands[2].shape[1]
    rank = operands[4].shape[1]
    vmem = pl.BlockSpec(memory_space=pltpu.VMEM)
    return pl.pallas_call(
        functools.partial(main_kernel, block_rows, total),
        out_shape=(
            pltpu.VMEM((rank, point_count), jnp.float32),
            pltpu.VMEM((point_count // LANES, LANES), jnp.float32),
            pltpu.VMEM((1, LANES), jnp.float32),
        ),
        in_specs=[vmem] * 5,
        out_specs=(vmem,) * 3,
        scratch_shapes=[
            pltpu.VMEM((12 * SUB, point_count), jnp.bfloat16),
            pltpu.VMEM((rank, LANES), jnp.float32),
            pltpu.VMEM((3 * rank, point_count), jnp.bfloat16),
        ],
        compiler_params=pltpu.CompilerParams(vmem_limit_bytes=24 << 20),
        name="factor_columns",
    )(*in_vmem(*operands))


def in_vmem(*values):
    return [pltpu.with_memory_space_constraint(value, pltpu.VMEM) for value in values]


def store_kernel(factor_ref, resid_ref, factor_out, resid_out, sems):
    rank = factor_ref.shape[0]
    count = sems.shape[0] - 1
    part = rank // count
    copies = [pltpu.make_async_copy(resid_ref, resid_out, sems.at[count])]
    for i in range(count):
        rows = slice(i * part, (i + 1) * part)
        copies.append(pltpu.make_async_copy(factor_ref.at[rows, :], factor_out.at[rows, :], sems.at[i]))
    for copy in copies:
        copy.start()
    for copy in copies:
        copy.wait()


def store_call(factor, resid):
    vmem = pl.BlockSpec(memory_space=pltpu.VMEM)
    hbm = pl.BlockSpec(memory_space=pl.ANY)
    return pl.pallas_call(
        store_kernel,
        out_shape=(jax.ShapeDtypeStruct(factor.shape, factor.dtype), jax.ShapeDtypeStruct(resid.shape, resid.dtype)),
        in_specs=[vmem] * 2,
        out_specs=(hbm,) * 2,
        scratch_shapes=[pltpu.SemaphoreType.DMA((9,))],
        cost_estimate=pl.CostEstimate(flops=4_000_000_000, bytes_accessed=2 * factor.size * 4, transcendentals=0),
        compiler_params=pltpu.CompilerParams(vmem_limit_bytes=1 << 20),
        name="store_factor",
    )(*in_vmem(factor, resid))


def to_chips(row, sizes):
    chips = math.prod(sizes[axis] for axis in CHIPS)
    return lax.all_to_all(jnp.broadcast_to(row[None], (chips,) + row.shape), CHIPS, 0, 0)


def of_chip(row):
    return row + lax.ppermute(row, CORES, ((0, 1), (1, 0)))


def body(sizes, points, scales, noise_var, pivots):
    dim, point_count = points.shape
    blocks, block_rows = pivots.shape
    devices = math.prod(sizes.values())
    chips = devices // sizes[CORES]
    noise = noise_var.reshape(point_count // LANES, LANES)
    vmem = pl.BlockSpec(memory_space=pltpu.VMEM)
    smem = pl.BlockSpec(memory_space=pltpu.SMEM)
    hbm = pl.BlockSpec(memory_space=pl.ANY)
    send, values, scaled, about, kept = pl.pallas_call(
        functools.partial(pre_kernel, sizes),
        out_shape=(
            pltpu.VMEM((1, LANES), jnp.float32),
            pltpu.VMEM((2 * SUB, LANES), jnp.float32),
            pltpu.VMEM((dim, point_count), jnp.float32),
            pltpu.VMEM((SUB, LANES), jnp.int32),
            pltpu.VMEM(noise.shape, jnp.float32),
        ),
        in_specs=[hbm] * 4,
        out_specs=(vmem,) * 5,
        scratch_shapes=[
            pltpu.VMEM((dim, point_count), jnp.float32),
            pltpu.SMEM((dim,), jnp.float32),
            pltpu.VMEM((blocks, block_rows), jnp.int32),
            pltpu.VMEM((SUB, LANES), jnp.int32),
            pltpu.SemaphoreType.DMA((4,)),
        ],
        name="pick_pivots",
    )(points, noise, scales, pivots)
    row = of_chip(send)
    last = lax.optimization_barrier(about[3, 0])
    got = to_chips(row, sizes).reshape(chips, LANES)

    def another(state):
        number, end, extra = state
        packed = pl.pallas_call(
            functools.partial(pack_kernel, sizes),
            out_shape=jax.ShapeDtypeStruct((1, LANES), jnp.float32),
            in_specs=[smem] + [vmem] * 2,
            out_specs=vmem,
            name="pack_more",
        )(number[None], values, about)
        more_got = to_chips(of_chip(packed), sizes).reshape(chips, LANES)
        extra = pl.pallas_call(
            unpack_kernel,
            out_shape=jax.ShapeDtypeStruct(extra.shape, jnp.float32),
            in_specs=[smem] + [vmem] * 3,
            out_specs=vmem,
            name="unpack_more",
        )(number[None], more_got, about, extra)
        return number + 1, end, extra

    start = (jnp.int32(1), last, jnp.zeros((2 * SUB, LANES), jnp.float32))
    extra = lax.while_loop(lambda state: state[0] <= state[1], another, start)[2]

    factor, resid, sums = factor_call(block_rows, devices * point_count, got, extra, scaled, kept, about)
    both = of_chip(sums)
    factor, resid = store_call(factor, resid)
    both, factor, resid = lax.optimization_barrier((both, factor, resid))
    means = jnp.sum(to_chips(both, sizes), axis=0)[0, :blocks]
    return factor, resid.reshape(point_count), means


def solution(mesh):
    split = Mesh(mesh.devices.reshape(4, 4, 8, 2), AXES)
    return jax.shard_map(
        functools.partial(body, dict(split.shape)),
        mesh=split,
        in_specs=(P(None, AXES), P(), P(AXES), P()),
        out_specs=(P(None, AXES), P(AXES), P()),
        check_vma=False,
    )
```

```python
import functools
import math

import jax
import jax.numpy as jnp
from jax import lax
from jax.experimental import pallas as pl
from jax.experimental.pallas import tpu as pltpu
from jax.sharding import Mesh
from jax.sharding import PartitionSpec as P


AXES = ("x", "y", "z", "c")
CHIPS = ("x", "y", "z")
CORES = "c"
LANES = 128
SUB = 8
ROOT = math.sqrt(0.5 * math.log2(math.e))
GRID = 16.0
SLOTS = 14


def iota(shape, dim):
    return lax.broadcasted_iota(jnp.int32, shape, dim)


def splat_row(tile, row):
    return jnp.broadcast_to(tile[row : row + 1, :], tile.shape)


def splat_col(tile, col):
    return jnp.broadcast_to(tile[:, col : col + 1], tile.shape)


def pivot_row(pivots_ref, wide_ref):
    blocks, block_rows = pivots_ref.shape
    wide_ref[...] = jnp.zeros_like(wide_ref)
    wide_ref[:, 0:block_rows] = pivots_ref[...]
    lane = iota((SUB, LANES), 1)
    spread = jnp.take_along_axis(wide_ref[...], lane % block_rows, axis=1, mode="promise_in_bounds")
    row = jnp.zeros((SUB, LANES), jnp.int32)
    for block in range(blocks):
        row = jnp.where(lane // block_rows == block, splat_row(spread, block), row)
    return row


def chip_index(sizes):
    chip = lax.axis_index(CHIPS[0])
    for axis in CHIPS[1:]:
        chip = chip * sizes[axis] + lax.axis_index(axis)
    return chip


def slots_of_lanes(rank, dim):
    lane = iota((rank, LANES), 1)
    slot = jnp.where(lane < dim * SLOTS, lane // dim, lane - dim * SLOTS)
    return jnp.where(slot < SLOTS, slot, -2 - 2 * rank).astype(jnp.float32)


def message(coords, noise, holds):
    dim = coords.shape[0]
    rank = holds.shape[0]
    index = jnp.sum(jnp.where(holds, iota((rank, LANES), 0) + 1, 0).astype(jnp.float32), axis=0, keepdims=True).astype(jnp.int32)
    index = jnp.broadcast_to(index, (SUB, LANES))
    taken = jnp.maximum(index - 1, 0)
    lane = iota((SUB, LANES), 1)
    place = jnp.where(lane < dim * SLOTS, lane % dim, dim)
    values = jnp.where(iota((SUB, LANES), 0) == place, jnp.take_along_axis(coords, taken, axis=1, mode="promise_in_bounds"), 0.0)
    row = jnp.sum(values, axis=0, keepdims=True)
    noises = jnp.take_along_axis(jnp.broadcast_to(noise, (SUB, LANES)), taken, axis=1, mode="promise_in_bounds")
    row = row + jnp.where(place == dim, noises, 0.0)[:1]
    return jnp.where(index[:1] > 0, row, 0.0)


def pre_kernel(
    sizes, points_hbm, noise_hbm, scales_hbm, pivots_hbm,
    send_ref, values_ref, scaled_ref, about_ref, kept_ref, points_ref, scales_ref, pivots_ref, wide_ref, sems,
):
    copies = []
    for i, (source, target) in enumerate(((pivots_hbm, pivots_ref), (points_hbm, points_ref), (noise_hbm, kept_ref), (scales_hbm, scales_ref))):
        copies.append(pltpu.make_async_copy(source, target, sems.at[i]))
        copies[i].start()
    dim, point_count = points_ref.shape
    tiles = point_count // LANES
    sub = iota((SUB, LANES), 0)
    lane = iota((SUB, LANES), 1)
    chip = chip_index(sizes)

    copies[0].wait()
    pivot = pivot_row(pivots_ref, wide_ref)
    rank = pivots_ref.shape[0] * pivots_ref.shape[1]
    local = pivot - (chip * sizes[CORES] + lax.axis_index(CORES)) * point_count
    owner = pivot // (point_count * sizes[CORES])
    owner_row = jnp.broadcast_to(owner[:1].astype(jnp.float32), (rank, LANES))
    owner_col = jnp.transpose(owner_row)
    same = owner_col == owner_row
    first, second = iota((rank, LANES), 0), iota((rank, LANES), 1)
    place_row = jnp.sum(jnp.where(same & (first < second), 1.0, 0.0), axis=0, keepdims=True)
    place_col = jnp.sum(jnp.where(same & (second < first), 1.0, 0.0), axis=1, keepdims=True)
    place = jnp.broadcast_to(place_row, (SUB, LANES))
    more = jnp.broadcast_to(jnp.max(place, axis=1, keepdims=True), (SUB, LANES)).astype(jnp.int32) // SLOTS
    about_ref[...] = jnp.where(sub == 0, local, jnp.where(sub == 1, owner, jnp.where(sub == 2, place.astype(jnp.int32), more)))
    mine = jnp.where(owner_col == chip.astype(jnp.float32), jnp.broadcast_to(place_col, (rank, LANES)), -1.0 - rank)
    holds = mine == slots_of_lanes(rank, dim)

    owned = (local >= 0) & (local < point_count)
    position = jnp.where(owned, local, -1)
    tile_of = position >> 7
    lane_of = position & (LANES - 1)
    for copy in copies[1:]:
        copy.wait()
    scale = jnp.zeros((SUB, LANES), jnp.float32)
    for d in range(dim):
        scale = jnp.where(sub == d, scales_ref[d], scale)
    factor = ROOT / scale
    coords = jnp.zeros((SUB, LANES), jnp.float32)
    for t in range(tiles):
        tile = points_ref[:, t * LANES : (t + 1) * LANES] * factor
        scaled_ref[:, t * LANES : (t + 1) * LANES] = tile
        found = jnp.take_along_axis(tile, lane_of, axis=1, mode="promise_in_bounds")
        coords = jnp.where(tile_of == t, found, coords)
    noise = jnp.zeros((SUB, LANES), jnp.float32)
    for a in range(tiles // SUB):
        found = jnp.take_along_axis(kept_ref[a * SUB : (a + 1) * SUB, :], lane_of, axis=1, mode="promise_in_bounds")
        noise = noise + jnp.where(tile_of == sub + a * SUB, found, 0.0)
    noise = jnp.sum(noise, axis=0, keepdims=True)
    values_ref[0:dim, :] = coords
    values_ref[dim:, :] = jnp.broadcast_to(noise, (SUB, LANES))
    send_ref[...] = message(coords, noise, holds)


def pack_kernel(sizes, number_ref, values_ref, about_ref, send_ref):
    dim = SUB
    rank = about_ref.shape[1]
    owner = jnp.transpose(jnp.broadcast_to(about_ref[1:2, :], (rank, LANES)).astype(jnp.float32))
    place = jnp.transpose(jnp.broadcast_to(about_ref[2:3, :], (rank, LANES)).astype(jnp.float32))
    first = (number_ref[0] * SLOTS).astype(jnp.float32)
    mine = jnp.where(owner == chip_index(sizes).astype(jnp.float32), place - first, -1.0 - rank)
    send_ref[...] = message(values_ref[0:dim, :], values_ref[dim : dim + 1, :], mine == slots_of_lanes(rank, dim))


def unpack(got, about_ref, number, dim):
    rank = about_ref.shape[1]
    chips = got.shape[0]
    owner = jnp.broadcast_to(about_ref[1:2, :], (chips, rank))
    slot = jnp.broadcast_to(about_ref[2:3, :], (SUB, rank)) - number * SLOTS
    pick = jnp.where(owner == iota((chips, rank), 0), 1.0, 0.0).astype(jnp.bfloat16)
    turned = jnp.concatenate(pieces(jnp.transpose(got)), axis=1)
    picked = jnp.dot(turned, jnp.concatenate([pick] * 3, axis=0), preferred_element_type=jnp.float32)
    coords = jnp.zeros((dim, rank), jnp.float32)
    for s in range(SLOTS):
        coords = jnp.where(slot == s, picked[s * dim : (s + 1) * dim, :], coords)
    noise = jnp.zeros((SUB, rank), jnp.float32)
    sub = iota((SUB, rank), 0)
    for at in range(dim * SLOTS, LANES, SUB):
        noise = noise + jnp.where((slot == sub + (at - dim * SLOTS)) & (slot < SLOTS), picked[at : at + SUB, :], 0.0)
    return coords, jnp.sum(noise, axis=0, keepdims=True)


def unpack_kernel(number_ref, got_ref, about_ref, before_ref, after_ref):
    dim = SUB
    coords, noise = unpack(got_ref[...], about_ref, number_ref[0], dim)
    after_ref[0:dim, :] = before_ref[0:dim, :] + coords
    after_ref[dim:, :] = before_ref[dim:, :] + noise


def pieces(value):
    high = value.astype(jnp.bfloat16)
    value = value - high.astype(jnp.float32)
    middle = value.astype(jnp.bfloat16)
    return high, middle, (value - middle.astype(jnp.float32)).astype(jnp.bfloat16)


def features(coords, second):
    _, count = coords.shape
    sub = iota((SUB, count), 0)
    coarse = jnp.round(coords * GRID)
    near = coarse * (1.0 / GRID)
    rest = coords - near
    low1 = rest.astype(jnp.bfloat16).astype(jnp.float32)
    left = rest - low1
    low2 = left.astype(jnp.bfloat16).astype(jnp.float32)
    low3 = left - low2
    square = jnp.sum(coarse * coarse, axis=0, keepdims=True)
    square_high = jnp.floor(square * (1.0 / 256)) * 256.0
    square_low = square - square_high
    mixed = jnp.sum(rest * (coords + near), axis=0, keepdims=True)
    mixed1 = mixed.astype(jnp.bfloat16).astype(jnp.float32)
    mixed2 = (mixed - mixed1).astype(jnp.bfloat16).astype(jnp.float32)
    mixed3 = mixed - mixed1 - mixed2

    def rows(*values):
        group = jnp.zeros((SUB, count), jnp.float32)
        for i, value in enumerate(values):
            group = jnp.where(sub == i, value, group)
        return group

    if second:
        return (
            coarse, rows(1.0, 1.0, square_high, square_low),
            low1, low2, low3, low1, low2, low1, near, near, near, rows(1.0, 1.0, 1.0, mixed1, mixed2, mixed3),
        )
    unit = -1.0 / (GRID * GRID)
    two = 2.0 * near
    return (
        coarse * (-2.0 * unit), rows(square_high * unit, square_low * unit, unit, unit),
        two, two, two, 2.0 * low1, 2.0 * low1, 2.0 * low2, 2.0 * low1, 2.0 * low2, 2.0 * low3,
        rows(-mixed1, -mixed2, -mixed3, -1.0, -1.0, -1.0),
    )


def exponent(left, right):
    return jnp.dot(left, right, preferred_element_type=jnp.float32)


def main_kernel(
    block_rows, total, got_ref, extra_ref, scaled_ref, noise_ref, about_ref,
    out_ref, resid_ref, sums_ref, side_ref, pair_ref, cov_ref,
):
    dim, point_count = scaled_ref.shape
    rank = pair_ref.shape[0]
    blocks = rank // block_rows
    halves = block_rows // SUB
    tiles_n = point_count // LANES
    width = 4 * LANES
    sub = iota((SUB, LANES), 0)
    lane = iota((SUB, LANES), 1)

    coords, noise_p = unpack(got_ref[...], about_ref, 0, dim)
    coords = coords + extra_ref[0:dim, :]
    noise_p = noise_p + extra_ref[dim : dim + 1, :]
    local = jnp.broadcast_to(about_ref[0:1, :], (SUB, LANES)).astype(jnp.float32)
    wanted = jnp.broadcast_to(jnp.transpose(local)[:, :1], (rank, LANES))
    pivot_side = jnp.transpose(jnp.concatenate(features(coords, False), axis=0)).astype(jnp.bfloat16)
    own_side = jnp.concatenate(features(coords, True), axis=0).astype(jnp.bfloat16)

    same = iota((rank, LANES), 0) == iota((rank, LANES), 1)
    pair_ref[...] = jnp.where(same, 1.0 + noise_p, jnp.exp2(exponent(pivot_side, own_side)))

    for t in range(tiles_n):
        groups = features(scaled_ref[:, t * LANES : (t + 1) * LANES], True)
        for i in range(0, len(groups), 2):
            pair = jnp.concatenate(groups[i : i + 2], axis=0).astype(jnp.bfloat16)
            side_ref[i * SUB : (i + 2) * SUB, t * LANES : (t + 1) * LANES] = pair

    for k in range(blocks):
        first = k * block_rows
        more = halves if k + 1 < blocks else 0
        tiles = [pair_ref[first + h * SUB : first + (h + 1) * SUB, :] for h in range(halves + more)]
        cols = [[splat_col(tile, first + j) for tile in tiles] for j in range(block_rows)]
        inside = (lane >= first) & (lane < first + block_rows)
        for h in range(halves + more):
            own = jnp.where(lane == sub + first + h * SUB, 1.0, 0.0)
            tiles[h] = jnp.where(inside, own if h < halves else 0.0, tiles[h])
        for m in range(block_rows):
            half, row = divmod(m, SUB)
            inv = lax.rsqrt(splat_row(cols[m][half], row))
            scaled_row = splat_row(tiles[half], row) * inv
            lower = [cols[m][h] * inv if h >= half else None for h in range(halves + more)]
            for j in range(m + 1, block_rows):
                half_j, row_j = divmod(j, SUB)
                entry = splat_row(lower[half_j], row_j)
                for h in range(half_j, halves + more):
                    cols[j][h] = cols[j][h] - lower[h] * entry
            for h in range(half, halves + more):
                if h == half:
                    below = tiles[h] - jnp.where(sub > row, lower[h], 0.0) * scaled_row
                    tiles[h] = jnp.where(sub == row, scaled_row, below)
                else:
                    tiles[h] = tiles[h] - lower[h] * scaled_row
        for h in range(halves + more):
            pair_ref[first + h * SUB : first + (h + 1) * SUB, :] = tiles[h]
        for t in range(k * tiles_n // blocks, (k + 1) * tiles_n // blocks, width // LANES):
            power = exponent(pivot_side, side_ref[:, t * LANES : t * LANES + width])
            for u in range(width // LANES):
                noisy = 1.0 + noise_ref[t + u : t + u + 1, :]
                ids = (iota((rank, LANES), 1) + (t + u) * LANES).astype(jnp.float32)
                tile = jnp.where(wanted == ids, noisy, jnp.exp2(power[:, u * LANES : (u + 1) * LANES]))
                high, middle, low = pieces(tile)
                for i, piece in enumerate((middle, high, low)):
                    cov_ref[i * rank : (i + 1) * rank, (t + u) * LANES : (t + u + 1) * LANES] = piece
        rest = first + 2 * block_rows
        if rest < rank:
            solved = jnp.concatenate(tiles[:halves], axis=0)
            high, middle, low = (piece.astype(jnp.float32) for piece in pieces(solved))
            turned = jnp.transpose(jnp.concatenate([high, high, middle, middle, low, high], axis=0)).astype(jnp.bfloat16)
            flat = jnp.concatenate([high, middle, high, middle, high, low], axis=0).astype(jnp.bfloat16)
            update = jnp.dot(turned[rest:, :], flat, preferred_element_type=jnp.float32)
            lane_r = iota((rank - rest, LANES), 1)
            inside_r = (lane_r >= first) & (lane_r < first + block_rows)
            pair_ref[rest:, :] = jnp.where(inside_r, 0.0, pair_ref[rest:, :]) - update

    inverse = jnp.where(iota((rank, LANES), 1) <= iota((rank, LANES), 0), pair_ref[...], 0.0)

    high, middle, low = pieces(inverse)
    stacked = jnp.concatenate([jnp.concatenate([high, high], axis=1), jnp.concatenate([middle, middle], axis=1)], axis=0)
    last = jnp.concatenate([low, high], axis=1)
    block_sums = [jnp.zeros((SUB, LANES), jnp.float32) for _ in range(blocks)]
    width = 8 * LANES
    for t in range(point_count // width):
        cols_t = slice(t * width, (t + 1) * width)
        large, small = cov_ref[: 2 * rank, cols_t], cov_ref[rank:, cols_t]
        both = jnp.dot(stacked, large, preferred_element_type=jnp.float32)
        new = (both[rank:, :] + jnp.dot(last, small, preferred_element_type=jnp.float32)) + both[:rank, :]
        out_ref[:, cols_t] = new
        for u in range(width // LANES):
            explained = None
            for b in range(blocks):
                part = None
                for h in range(halves):
                    at = b * block_rows + h * SUB
                    tile = new[at : at + SUB, u * LANES : (u + 1) * LANES]
                    part = tile * tile if part is None else part + tile * tile
                block_sums[b] = block_sums[b] + part
                explained = part if explained is None else explained + part
            row = t * (width // LANES) + u
            resid_ref[row : row + 1, :] = (1.0 + noise_ref[row : row + 1, :]) - jnp.sum(explained, axis=0, keepdims=True)

    running = None
    for a in range(tiles_n // SUB):
        tile = 1.0 + noise_ref[a * SUB : (a + 1) * SUB, :]
        running = tile if running is None else running + tile
    means = jnp.zeros((SUB, LANES), jnp.float32)
    for b in range(blocks):
        running = running - block_sums[b]
        means = jnp.where(sub == b, jnp.broadcast_to(jnp.sum(running, axis=0, keepdims=True), (SUB, LANES)), means)
    means = jnp.broadcast_to(jnp.sum(means, axis=1, keepdims=True), (SUB, LANES)) * (1.0 / total)
    sums_ref[...] = jnp.broadcast_to(jnp.sum(jnp.where(sub == lane, means, 0.0), axis=0, keepdims=True), sums_ref.shape)


def factor_call(block_rows, total, *operands):
    point_count = operands[2].shape[1]
    rank = operands[4].shape[1]
    vmem = pl.BlockSpec(memory_space=pltpu.VMEM)
    return pl.pallas_call(
        functools.partial(main_kernel, block_rows, total),
        out_shape=(
            pltpu.VMEM((rank, point_count), jnp.float32),
            pltpu.VMEM((point_count // LANES, LANES), jnp.float32),
            pltpu.VMEM((1, LANES), jnp.float32),
        ),
        in_specs=[vmem] * 5,
        out_specs=(vmem,) * 3,
        scratch_shapes=[
            pltpu.VMEM((12 * SUB, point_count), jnp.bfloat16),
            pltpu.VMEM((rank, LANES), jnp.float32),
            pltpu.VMEM((3 * rank, point_count), jnp.bfloat16),
        ],
        compiler_params=pltpu.CompilerParams(vmem_limit_bytes=24 << 20),
        name="factor_columns",
    )(*in_vmem(*operands))


def in_vmem(*values):
    return [pltpu.with_memory_space_constraint(value, pltpu.VMEM) for value in values]


def store_kernel(factor_ref, resid_ref, factor_out, resid_out, sems):
    rank = factor_ref.shape[0]
    count = sems.shape[0] - 1
    part = rank // count
    copies = [pltpu.make_async_copy(resid_ref, resid_out, sems.at[count])]
    for i in range(count):
        rows = slice(i * part, (i + 1) * part)
        copies.append(pltpu.make_async_copy(factor_ref.at[rows, :], factor_out.at[rows, :], sems.at[i]))
    for copy in copies:
        copy.start()
    for copy in copies:
        copy.wait()


def store_call(factor, resid):
    vmem = pl.BlockSpec(memory_space=pltpu.VMEM)
    hbm = pl.BlockSpec(memory_space=pl.ANY)
    return pl.pallas_call(
        store_kernel,
        out_shape=(jax.ShapeDtypeStruct(factor.shape, factor.dtype), jax.ShapeDtypeStruct(resid.shape, resid.dtype)),
        in_specs=[vmem] * 2,
        out_specs=(hbm,) * 2,
        scratch_shapes=[pltpu.SemaphoreType.DMA((9,))],
        cost_estimate=pl.CostEstimate(flops=4_000_000_000, bytes_accessed=2 * factor.size * 4, transcendentals=0),
        compiler_params=pltpu.CompilerParams(vmem_limit_bytes=1 << 20),
        name="store_factor",
    )(*in_vmem(factor, resid))


def to_chips(row, sizes):
    chips = math.prod(sizes[axis] for axis in CHIPS)
    return lax.all_to_all(jnp.broadcast_to(row[None], (chips,) + row.shape), CHIPS, 0, 0)


def of_chip(row):
    return row + lax.ppermute(row, CORES, ((0, 1), (1, 0)))


def body(sizes, points, scales, noise_var, pivots):
    dim, point_count = points.shape
    blocks, block_rows = pivots.shape
    devices = math.prod(sizes.values())
    chips = devices // sizes[CORES]
    noise = noise_var.reshape(point_count // LANES, LANES)
    vmem = pl.BlockSpec(memory_space=pltpu.VMEM)
    smem = pl.BlockSpec(memory_space=pltpu.SMEM)
    hbm = pl.BlockSpec(memory_space=pl.ANY)
    send, values, scaled, about, kept = pl.pallas_call(
        functools.partial(pre_kernel, sizes),
        out_shape=(
            pltpu.VMEM((1, LANES), jnp.float32),
            pltpu.VMEM((2 * SUB, LANES), jnp.float32),
            pltpu.VMEM((dim, point_count), jnp.float32),
            pltpu.VMEM((SUB, LANES), jnp.int32),
            pltpu.VMEM(noise.shape, jnp.float32),
        ),
        in_specs=[hbm] * 4,
        out_specs=(vmem,) * 5,
        scratch_shapes=[
            pltpu.VMEM((dim, point_count), jnp.float32),
            pltpu.SMEM((dim,), jnp.float32),
            pltpu.VMEM((blocks, block_rows), jnp.int32),
            pltpu.VMEM((SUB, LANES), jnp.int32),
            pltpu.SemaphoreType.DMA((4,)),
        ],
        name="pick_pivots",
    )(points, noise, scales, pivots)
    row = of_chip(send)
    last = lax.optimization_barrier(about[3, 0])
    got = to_chips(row, sizes).reshape(chips, LANES)

    def another(state):
        number, end, extra = state
        packed = pl.pallas_call(
            functools.partial(pack_kernel, sizes),
            out_shape=jax.ShapeDtypeStruct((1, LANES), jnp.float32),
            in_specs=[smem] + [vmem] * 2,
            out_specs=vmem,
            name="pack_more",
        )(number[None], values, about)
        more_got = to_chips(of_chip(packed), sizes).reshape(chips, LANES)
        extra = pl.pallas_call(
            unpack_kernel,
            out_shape=jax.ShapeDtypeStruct(extra.shape, jnp.float32),
            in_specs=[smem] + [vmem] * 3,
            out_specs=vmem,
            name="unpack_more",
        )(number[None], more_got, about, extra)
        return number + 1, end, extra

    start = (jnp.int32(1), last, jnp.zeros((2 * SUB, LANES), jnp.float32))
    extra = lax.while_loop(lambda state: state[0] <= state[1], another, start)[2]

    factor, resid, sums = factor_call(block_rows, devices * point_count, got, extra, scaled, kept, about)
    both = of_chip(sums)
    factor, resid = store_call(factor, resid)
    both, factor, resid = lax.optimization_barrier((both, factor, resid))
    means = jnp.sum(to_chips(both, sizes), axis=0)[0, :blocks]
    return factor, resid.reshape(point_count), means


def solution(mesh):
    split = Mesh(mesh.devices.reshape(4, 4, 8, 2), AXES)
    return jax.shard_map(
        functools.partial(body, dict(split.shape)),
        mesh=split,
        in_specs=(P(None, AXES), P(), P(AXES), P()),
        out_specs=(P(None, AXES), P(AXES), P()),
        check_vma=False,
    )
```
